768 devices in a mesh: curve: 96 (over z, x, core), level: 8 (over y).
Axes of the slice: x: 4, y: 8, z: 12, core: 2. Of those that a mesh axis runs over, the one named last changes fastest.
Arguments:
- right_side: float32 [512, 98304], P(None, ('curve', 'level')), may hold values from -6 to 6
- counts: int32 [768], replicated, may hold values from 96 to 128, as said below
- neighbours: int32 [6, 98304], P(None, ('curve', 'level')), may hold values from -1 to 98303, as said below
Outputs:
- solution: float32 [512, 98304], P(None, ('curve', 'level'))
- residual: float32 [512, 98304], P(None, ('curve', 'level'))
- residual_norm: float32 [], replicated
The draws below stay inside these ranges and needn't reach their ends.
Inputs may be any that keep to these rules, and one draw needn't show every extreme that they name: `counts`: some device holds 128 live bricks and some device holds 96. `neighbours`: A slot's global number is its device times 128 plus its position. The relation is symmetric across opposite faces; padding slots have -1 on every face and no brick names them. Live bricks are numbered along the curve; the brick across face 0, 2 or 4 lies earlier on the curve and the one across face 1, 3 or 5 later, at most 256 live bricks away.
All inputs are finite; a program needn't handle non-finite values.
Results may differ from the reference program's by a relative error of at most 0.00027.
Values sent between devices are 32-bit elements; how exact they have to be, the bound alone decides.
No kernel may reach another device: no remote copies, remote signals or barrier semaphores. Data moves between devices by JAX's collectives and lax.ppermute only.
A program may use at most 32 MiB of HBM per device.

```python
import jax
import jax.numpy as jnp
from jax import lax

SLOT_DEV = 128
MIN_LIVE = 96
SIDE = 16
LAYER = 256
CELLS = 512
SLOTS = 98304


def brick_layout(key):
    device_total = SLOTS // SLOT_DEV
    counts = jax.random.randint(jax.random.fold_in(key, 11), (device_total,), MIN_LIVE, SLOT_DEV + 1)
    fullest = jax.random.randint(jax.random.fold_in(key, 12), (), 0, device_total)
    emptiest = (fullest + 1 + jax.random.randint(jax.random.fold_in(key, 13), (), 0, device_total - 1)) % device_total
    device_ids = jnp.arange(device_total)
    counts = jnp.where(device_ids == fullest, SLOT_DEV, counts)
    counts = jnp.where(device_ids == emptiest, MIN_LIVE, counts)
    return counts.astype(jnp.int32)


def morton_split(morton):
    coord_x = jnp.zeros_like(morton)
    coord_y = jnp.zeros_like(morton)
    for bit_index in range(8):
        coord_x = coord_x | (morton >> 2 * bit_index & 1) << bit_index
        coord_y = coord_y | (morton >> 2 * bit_index + 1 & 1) << bit_index
    return (coord_x, coord_y)


def morton_join(coord_x, coord_y):
    morton = jnp.zeros_like(coord_x)
    for bit_index in range(8):
        morton = morton | (coord_x >> bit_index & 1) << 2 * bit_index
        morton = morton | (coord_y >> bit_index & 1) << 2 * bit_index + 1
    return morton


def draw_counts(key, part):
    return brick_layout(key)


def draw_neighbours(key, part):
    counts = brick_layout(key)
    starts = (jnp.cumsum(counts) - counts).astype(jnp.int32)
    total_live = jnp.sum(counts).astype(jnp.int32)
    slot_ids = jnp.arange(SLOTS, dtype=jnp.int32)
    device_of = slot_ids // SLOT_DEV
    offset = slot_ids % SLOT_DEV
    live_slot = offset < counts[device_of]
    live_index = starts[device_of] + offset
    layer_index = live_index // LAYER
    coord_x, coord_y = morton_split(live_index % LAYER)
    columns = []
    for step_x, step_y, step_z in [(-1, 0, 0), (1, 0, 0), (0, -1, 0), (0, 1, 0), (0, 0, -1), (0, 0, 1)]:
        next_x = coord_x + step_x
        next_y = coord_y + step_y
        next_z = layer_index + step_z
        inside = (next_x >= 0) & (next_x < SIDE) & (next_y >= 0) & (next_y < SIDE) & (next_z >= 0)
        other = next_z * LAYER + morton_join(jnp.clip(next_x, 0, SIDE - 1), jnp.clip(next_y, 0, SIDE - 1))
        inside = inside & (other < total_live) & live_slot
        other = jnp.clip(other, 0, total_live - 1)
        owner = (jnp.searchsorted(starts, other, side='right') - 1).astype(jnp.int32)
        global_slot = owner * SLOT_DEV + other - starts[owner]
        columns.append(jnp.where(inside, global_slot, -1))
    return jnp.stack(columns).astype(jnp.int32)


def shard_levels(key, shape, split, least, high):
    loudness = 1.0
    for axis_at, shards_of in split:
        draws = jax.random.uniform(jax.random.fold_in(jax.random.fold_in(key, 6), axis_at), (shards_of,), jnp.float32, least / len(split), high / len(split))
        loudness = loudness * jnp.repeat(jnp.exp(draws), shape[axis_at] // shards_of).reshape((-1,) + (1,) * (len(shape) - 1 - axis_at))
    return loudness


def bell_draw(stream_key, dims, width, limit, pieces=(), kind=jnp.bfloat16):
    drawn = width * jax.random.normal(stream_key, dims, jnp.float32)
    if pieces:
        drawn = drawn * shard_levels(stream_key, dims, pieces, -0.22, 0.18)
    return jnp.clip(drawn, -limit, limit).astype(kind)


def setup_inputs(seed: int = 0) -> dict:
    arg_keys = jax.random.split(jax.random.key(seed), 4)
    right_side = bell_draw(arg_keys[0], (CELLS, SLOTS), 1.0, 6.0, ((1, 768),), jnp.float32)
    counts = draw_counts(jax.random.fold_in(arg_keys[3], 71), 0)
    neighbours = draw_neighbours(jax.random.fold_in(arg_keys[3], 71), 0)
    return {"right_side": right_side, "counts": counts, "neighbours": neighbours}


OPPOSITE = (1, 0, 3, 2, 5, 4)
RELAXATION = 2.0 / 3.0

def brick_faces(values, extent):
    volume = values.reshape(extent, extent, extent, -1)
    surfaces = [volume[0], volume[extent - 1], volume[:, 0], volume[:, extent - 1], volume[:, :, 0], volume[:, :, extent - 1]]
    return jnp.stack([one_face.reshape(extent * extent, -1) for one_face in surfaces])

def gather_ghosts(lookup, position, present):
    ghosts = []
    for face_id in range(6):
        picked = jnp.take(lookup[OPPOSITE[face_id]], position[face_id], axis=1)
        ghosts.append(jnp.where(present[face_id][None, :], picked, jnp.zeros_like(picked)))
    return ghosts

def apply_operator(values, ghosts, extent, weight):
    brick_count = values.shape[1]
    volume = values.reshape(extent, extent, extent, brick_count)
    padded = jnp.pad(volume, ((1, 1), (1, 1), (1, 1), (0, 0)))
    shaped = [ghost.reshape(extent, extent, brick_count) for ghost in ghosts]
    padded = padded.at[0, 1:-1, 1:-1].set(shaped[0])
    padded = padded.at[-1, 1:-1, 1:-1].set(shaped[1])
    padded = padded.at[1:-1, 0, 1:-1].set(shaped[2])
    padded = padded.at[1:-1, -1, 1:-1].set(shaped[3])
    padded = padded.at[1:-1, 1:-1, 0].set(shaped[4])
    padded = padded.at[1:-1, 1:-1, -1].set(shaped[5])
    beside = padded[2:, 1:-1, 1:-1] + padded[:-2, 1:-1, 1:-1]
    beside = beside + padded[1:-1, 2:, 1:-1] + padded[1:-1, :-2, 1:-1]
    beside = beside + padded[1:-1, 1:-1, 2:] + padded[1:-1, 1:-1, :-2]
    return ((6.0 * volume - beside) * weight).reshape(extent * extent * extent, brick_count)

def restrict(values):
    brick_count = values.shape[1]
    grouped = values.reshape(4, 2, 4, 2, 4, 2, brick_count)
    return lax.optimization_barrier(jnp.mean(grouped, axis=(1, 3, 5))).reshape(64, brick_count)

def prolong(coarse):
    brick_count = coarse.shape[1]
    spread = jnp.broadcast_to(coarse.reshape(4, 1, 4, 1, 4, 1, brick_count), (4, 2, 4, 2, 4, 2, brick_count))
    return spread.reshape(512, brick_count)

def precondition(residual_in, exchange):
    relax_fine = RELAXATION / 6.0
    relax_coarse = RELAXATION / 1.5
    sweep_one = relax_fine * residual_in
    sweep_two = sweep_one + relax_fine * (residual_in - apply_operator(sweep_one, exchange(brick_faces(sweep_one, 8)), 8, 1.0))
    defect = residual_in - apply_operator(sweep_two, exchange(brick_faces(sweep_two, 8)), 8, 1.0)
    coarse_rhs = restrict(defect)
    coarse_one = relax_coarse * coarse_rhs
    coarse_two = coarse_one + relax_coarse * (coarse_rhs - apply_operator(coarse_one, exchange(brick_faces(coarse_one, 4)), 4, 0.25))
    sweep_three = sweep_two + prolong(coarse_two)
    return sweep_three + relax_fine * (residual_in - apply_operator(sweep_three, exchange(brick_faces(sweep_three, 8)), 8, 1.0))

def reference(right_side, counts, neighbours):
    slot_ids = jnp.arange(SLOTS, dtype=jnp.int32)
    live_slot = slot_ids % SLOT_DEV < counts[slot_ids // SLOT_DEV]
    residual_in = jnp.where(live_slot[None, :], right_side, jnp.zeros_like(right_side))
    present = neighbours >= 0
    position = jnp.where(present, neighbours, 0).astype(jnp.int32)

    def exchange(surface):
        return gather_ghosts(surface, position, present)
    preconditioned = precondition(residual_in, exchange)
    image = apply_operator(preconditioned, exchange(brick_faces(preconditioned, 8)), 8, 1.0)
    along = jnp.sum(residual_in * preconditioned)
    curvature = jnp.sum(preconditioned * image)
    step_size = along / curvature
    solution = step_size * preconditioned
    residual = residual_in - step_size * image
    residual_norm = jnp.sqrt(jnp.sum(residual * residual))
    return (solution, residual, residual_norm)
```

```python
import functools

import jax
import jax.numpy as jnp
from jax import lax
from jax.experimental import pallas as pl
from jax.experimental.pallas import tpu as pltpu
from jax.sharding import Mesh
from jax.sharding import PartitionSpec as P

LANES = 128
TAIL = 64
FINE = 192
COARSE = 48
GROUP = 16
AXES = ("outer", "inner")
RELAX_FINE = (2.0 / 3.0) / 6.0
RELAX_COARSE = (2.0 / 3.0) / 1.5

VMEM = pl.BlockSpec(memory_space=pltpu.VMEM)
SMEM = pl.BlockSpec(memory_space=pltpu.SMEM)

LANE_ROW = 0
WINDOW_ROW = 8
FORWARD_UP = 16
FORWARD_DOWN = 24
TABLE_ROWS = 32


def f32(*shape):
    return jax.ShapeDtypeStruct(shape, jnp.float32)


def i32(*shape):
    return jax.ShapeDtypeStruct(shape, jnp.int32)


def call(kernel, name, outs, *args, in_specs=None, out_specs=None, scratch=()):
    return pl.pallas_call(
        kernel,
        out_shape=outs,
        in_specs=in_specs or [VMEM] * len(args),
        out_specs=out_specs or [VMEM] * len(outs),
        scratch_shapes=list(scratch),
        name=name,
    )(*args)


def take(block, lanes):
    return jnp.take_along_axis(block, lanes, axis=1, mode="promise_in_bounds")


def write_faces(values, up, down):
    up[0:64, :] = values[448:512, :]
    down[0:64, :] = values[0:64, :]
    for x in range(8):
        up[64 + 8 * x : 72 + 8 * x, :] = values[64 * x + 56 : 64 * x + 64, :]
        down[64 + 8 * x : 72 + 8 * x, :] = values[64 * x : 64 * x + 8, :]
    up[128:192, :] = values[pl.ds(7, 64, stride=8), :]
    down[128:192, :] = values[pl.ds(0, 64, stride=8), :]


def write_coarse_faces(values, up, down):
    up[0:16, :] = values[48:64, :]
    down[0:16, :] = values[0:16, :]
    for x in range(4):
        up[16 + 4 * x : 20 + 4 * x, :] = values[16 * x + 12 : 16 * x + 16, :]
        down[16 + 4 * x : 20 + 4 * x, :] = values[16 * x : 16 * x + 4, :]
    up[32:48, :] = values[pl.ds(3, 16, stride=4), :]
    down[32:48, :] = values[pl.ds(0, 16, stride=4), :]


def read_ghosts(table, windows, ghosts, rows):
    per_face = rows // 3
    packed = rows // 2
    for face in range(6):
        own, near, far = windows[face % 2]
        lane = jnp.broadcast_to(table[LANE_ROW + face : LANE_ROW + face + 1, :], (8, LANES))
        window = jnp.broadcast_to(table[WINDOW_ROW + face : WINDOW_ROW + face + 1, :], (8, LANES))
        is_own, is_near, is_far, is_last = [window == which for which in range(4)]
        first_half = jnp.minimum(lane, TAIL - 1)
        second_half = first_half + TAIL
        for step in range(0, per_face, 8):
            row = (face // 2) * per_face + step
            last_row = rows + row % packed
            last_lane = first_half if row < packed else second_half
            picked = jnp.where(is_last, take(far[last_row : last_row + 8, :], last_lane), 0.0)
            picked = jnp.where(is_far, take(far[row : row + 8, :], lane), picked)
            picked = jnp.where(is_near, take(near[row : row + 8, :], lane), picked)
            picked = jnp.where(is_own, take(own[row : row + 8, :], lane), picked)
            ghosts[face * per_face + step : face * per_face + step + 8, :] = picked


def beside(values, ghosts, x, y):
    sub = lax.broadcasted_iota(jnp.int32, (8, LANES), 0)
    at = 64 * x + 8 * y
    line = 8 * x + y
    centre = values[at : at + 8, :]
    below_x = values[at - 64 : at - 56, :] if x > 0 else ghosts[8 * y : 8 * y + 8, :]
    above_x = values[at + 64 : at + 72, :] if x < 7 else ghosts[64 + 8 * y : 72 + 8 * y, :]
    below_y = values[at - 8 : at, :] if y > 0 else ghosts[128 + 8 * x : 136 + 8 * x, :]
    above_y = values[at + 8 : at + 16, :] if y < 7 else ghosts[192 + 8 * x : 200 + 8 * x, :]
    below_z = jnp.where(sub == 0, ghosts[256 + line : 257 + line, :], pltpu.roll(centre, 1, 0))
    above_z = jnp.where(sub == 7, ghosts[320 + line : 321 + line, :], pltpu.roll(centre, 7, 0))
    return centre, ((above_x + below_x) + (above_y + below_y)) + (above_z + below_z)


def start_kernel(device_ref, counts_ref, right_ref, neighbours_ref, residual, up, down, table):
    device = device_ref[0]
    own_count = counts_ref[device]
    lane = lax.broadcasted_iota(jnp.int32, (8, LANES), 1)
    live = lane < own_count
    for row in range(0, 512, 8):
        residual[row : row + 8, :] = jnp.where(live, right_ref[row : row + 8, :], 0.0)
    write_faces(residual, up, down)
    slot = neighbours_ref[...]
    present = slot >= 0
    slot = jnp.where(present, slot, 0)
    distance = jnp.abs(lax.shift_right_logical(slot, 7) - device)
    offset = slot & (LANES - 1)
    face = lax.broadcasted_iota(jnp.int32, (6, LANES), 0)
    skipped = jnp.maximum(counts_ref[jnp.maximum(device - 3, 0)] - TAIL, 0)
    shifted = jnp.where((distance == 3) & (face % 2 == 0), offset - skipped, offset)
    table[LANE_ROW : LANE_ROW + 6, :] = jnp.clip(shifted, 0, LANES - 1)
    table[WINDOW_ROW : WINDOW_ROW + 6, :] = jnp.where(present, distance, -1)
    forward = jnp.maximum(counts_ref[jnp.maximum(device - 1, 0)] - TAIL, 0)
    table[FORWARD_UP : FORWARD_UP + 8, :] = (lane & (TAIL - 1)) + forward
    table[FORWARD_DOWN : FORWARD_DOWN + 8, :] = lane & (TAIL - 1)


def pack_kernel(rows, forward_row, own, received, table, message):
    half = rows // 2
    lane = lax.broadcasted_iota(jnp.int32, (8, LANES), 1)
    forward = table[forward_row : forward_row + 8, :]
    message[0:rows, :] = own[...]
    for row in range(0, half, 8):
        first = take(received[row : row + 8, :], forward)
        second = take(received[half + row : half + row + 8, :], forward)
        message[rows + row : rows + row + 8, :] = jnp.where(lane < TAIL, first, second)


def smooth_kernel(residual, up, down, near_up, far_up, near_down, far_down, table, out, out_up, out_down, ghosts):
    read_ghosts(table, ((up, near_up, far_up), (down, near_down, far_down)), ghosts, FINE)
    for x in range(8):
        for y in range(8):
            centre, around = beside(residual, ghosts, x, y)
            first = RELAX_FINE * centre
            applied = 6.0 * first - RELAX_FINE * around
            at = 64 * x + 8 * y
            out[at : at + 8, :] = first + RELAX_FINE * (centre - applied)
    write_faces(out, out_up, out_down)


def defect_kernel(
    residual, second, up, down, near_up, far_up, near_down, far_down, table,
    defect, coarse, out_up, out_down, ghosts, sums, scaled,
):
    read_ghosts(table, ((up, near_up, far_up), (down, near_down, far_down)), ghosts, FINE)
    for big_x in range(4):
        for big_y in range(4):
            total = None
            for x in (2 * big_x, 2 * big_x + 1):
                for y in (2 * big_y, 2 * big_y + 1):
                    centre, around = beside(second, ghosts, x, y)
                    at = 64 * x + 8 * y
                    part = residual[at : at + 8, :] - (6.0 * centre - around)
                    defect[at : at + 8, :] = part
                    total = part if total is None else total + part
            at = 32 * big_x + 8 * big_y
            sums[at : at + 8, :] = total
    restricted = (sums[pl.ds(0, 64, stride=2), :] + sums[pl.ds(1, 64, stride=2), :]) * 0.125
    coarse[...] = restricted
    scaled[...] = RELAX_COARSE * restricted
    write_coarse_faces(scaled, out_up, out_down)


def coarse_kernel(
    coarse, up, down, near_up, far_up, near_down, far_down, table,
    out, out_up, out_down, ghosts, low_y, high_y, low_z, high_z,
):
    read_ghosts(table, ((up, near_up, far_up), (down, near_down, far_down)), ghosts, COARSE)
    for x in range(4):
        low_y[16 * x : 16 * x + 4, :] = ghosts[32 + 4 * x : 36 + 4 * x, :]
        high_y[16 * x + 12 : 16 * x + 16, :] = ghosts[48 + 4 * x : 52 + 4 * x, :]
    low_z[pl.ds(0, 16, stride=4), :] = ghosts[64:80, :]
    high_z[pl.ds(3, 16, stride=4), :] = ghosts[80:96, :]
    rhs = coarse[...]
    first = RELAX_COARSE * rhs
    row = lax.broadcasted_iota(jnp.int32, (64, LANES), 0)
    below_x = jnp.concatenate([ghosts[0:16, :], first[0:48, :]], axis=0)
    above_x = jnp.concatenate([first[16:64, :], ghosts[16:32, :]], axis=0)
    below_y = jnp.where((row & 15) < 4, low_y[...], pltpu.roll(first, 4, 0))
    above_y = jnp.where((row & 15) >= 12, high_y[...], pltpu.roll(first, 60, 0))
    below_z = jnp.where((row & 3) == 0, low_z[...], pltpu.roll(first, 1, 0))
    above_z = jnp.where((row & 3) == 3, high_z[...], pltpu.roll(first, 63, 0))
    around = ((above_x + below_x) + (above_y + below_y)) + (above_z + below_z)
    out[...] = first + RELAX_COARSE * (rhs - (6.0 * first - around) * 0.25)
    write_coarse_faces(out, out_up, out_down)


def correct_kernel(
    second, defect, coarse, up, down, near_up, far_up, near_down, far_down, table,
    out, out_up, out_down, ghosts, wide, wide_ghosts, spread,
):
    read_ghosts(table, ((up, near_up, far_up), (down, near_down, far_down)), ghosts, COARSE)
    wide[pl.ds(0, 64, stride=2), :] = coarse[...]
    wide[pl.ds(1, 64, stride=2), :] = coarse[...]
    wide_ghosts[pl.ds(0, 64, stride=2), :] = ghosts[0:64, :]
    wide_ghosts[pl.ds(1, 64, stride=2), :] = ghosts[0:64, :]
    for x in range(8):
        for y in range(8):
            at = 64 * x + 8 * y
            source = 32 * (x // 2) + 8 * (y // 2)
            spread[at : at + 8, :] = wide[source : source + 8, :]
    sub = lax.broadcasted_iota(jnp.int32, (8, LANES), 0)
    for x in range(8):
        for y in range(8):
            at = 64 * x + 8 * y
            cell = 4 * (x // 2) + y // 2
            centre = spread[at : at + 8, :]
            side_x = 8 * (y // 2)
            side_y = 8 * (x // 2)
            below_x = spread[at - 64 : at - 56, :] if x > 0 else wide_ghosts[side_x : side_x + 8, :]
            above_x = spread[at + 64 : at + 72, :] if x < 7 else wide_ghosts[32 + side_x : 40 + side_x, :]
            below_y = spread[at - 8 : at, :] if y > 0 else wide_ghosts[64 + side_y : 72 + side_y, :]
            above_y = spread[at + 8 : at + 16, :] if y < 7 else wide_ghosts[96 + side_y : 104 + side_y, :]
            below_z = jnp.where(sub == 0, ghosts[64 + cell : 65 + cell, :], pltpu.roll(centre, 1, 0))
            above_z = jnp.where(sub == 7, ghosts[80 + cell : 81 + cell, :], pltpu.roll(centre, 7, 0))
            around = ((above_x + below_x) + (above_y + below_y)) + (above_z + below_z)
            left = defect[at : at + 8, :] - (6.0 * centre - around)
            out[at : at + 8, :] = (second[at : at + 8, :] + centre) + RELAX_FINE * left
    write_faces(out, out_up, out_down)


def image_kernel(residual, direction, up, down, near_up, far_up, near_down, far_down, table, image, sums, ghosts):
    read_ghosts(table, ((up, near_up, far_up), (down, near_down, far_down)), ghosts, FINE)
    zero = jnp.zeros((8, LANES), jnp.float32)
    parts = [zero] * 5
    for x in range(8):
        for y in range(8):
            centre, around = beside(direction, ghosts, x, y)
            at = 64 * x + 8 * y
            applied = 6.0 * centre - around
            image[at : at + 8, :] = applied
            start = residual[at : at + 8, :]
            terms = (start * centre, centre * applied, start * start, start * applied, applied * applied)
            parts = [part + term for part, term in zip(parts, terms)]
    lane = lax.broadcasted_iota(jnp.int32, (1, LANES), 1)
    row = jnp.zeros((1, LANES), jnp.float32)
    for index, part in enumerate(parts):
        row = jnp.where(lane == index, jnp.sum(part), row)
    for copy in range(sums.shape[0]):
        sums[copy] = row


def add_kernel(received, out):
    total = received[0]
    for index in range(1, received.shape[0]):
        total = total + received[index]
    for copy in range(out.shape[0]):
        out[copy] = total


def finish_kernel(received, residual, direction, image, solution, left, norm):
    total = received[0]
    for index in range(1, received.shape[0]):
        total = total + received[index]
    lane = lax.broadcasted_iota(jnp.int32, (1, LANES), 1)
    along, curvature, old_square, cross_term, image_square = [
        jnp.full((8, LANES), jnp.sum(jnp.where(lane == index, total, 0.0)), jnp.float32) for index in range(5)
    ]
    step_size = along / curvature
    for row in range(0, 512, 8):
        solution[row : row + 8, :] = step_size * direction[row : row + 8, :]
        left[row : row + 8, :] = residual[row : row + 8, :] - step_size * image[row : row + 8, :]
    norm[...] = jnp.sqrt(old_square - 2.0 * step_size * cross_term + step_size * step_size * image_square)


def shift(block, distance):
    count = lax.axis_size(AXES)
    route = [(i, i + distance) for i in range(count) if 0 <= i + distance < count]
    return lax.ppermute(block, AXES, route)


def exchange(up, down, table, rows):
    near_up = shift(up, 1)
    near_down = shift(down, -1)
    message = [f32(rows + rows // 2, LANES)]
    (message_up,) = call(functools.partial(pack_kernel, rows, FORWARD_UP), "pack_up", message, up, near_up, table)
    far_up = shift(message_up, 2)
    (message_down,) = call(
        functools.partial(pack_kernel, rows, FORWARD_DOWN), "pack_down", message, down, near_down, table
    )
    far_down = shift(message_down, -2)
    return up, down, near_up, far_up, near_down, far_down, table


def local(right_side, counts, neighbours):
    device = lax.axis_index(AXES).astype(jnp.int32).reshape(1)
    fine = f32(512, LANES)
    faces = [f32(FINE, LANES)] * 2
    coarse = f32(64, LANES)
    coarse_faces = [f32(COARSE, LANES)] * 2
    fine_ghosts = pltpu.VMEM((2 * FINE, LANES), jnp.float32)
    coarse_ghosts = pltpu.VMEM((2 * COARSE, LANES), jnp.float32)
    scratch = lambda rows: pltpu.VMEM((rows, LANES), jnp.float32)

    residual_in, up, down, table = call(
        start_kernel, "start", [fine, *faces, i32(TABLE_ROWS, LANES)], device, counts, right_side, neighbours,
        in_specs=[SMEM, SMEM, VMEM, VMEM],
    )
    second, up, down = call(
        smooth_kernel, "smooth", [fine, *faces], residual_in, *exchange(up, down, table, FINE), scratch=[fine_ghosts]
    )
    defect, rhs, up, down = call(
        defect_kernel, "defect", [fine, coarse, *coarse_faces],
        residual_in, second, *exchange(up, down, table, FINE), scratch=[fine_ghosts, scratch(128), scratch(64)],
    )
    correction, up, down = call(
        coarse_kernel, "coarse", [coarse, *coarse_faces],
        rhs, *exchange(up, down, table, COARSE), scratch=[coarse_ghosts] + [scratch(64)] * 4,
    )
    direction, up, down = call(
        correct_kernel, "correct", [fine, *faces],
        second, defect, correction, *exchange(up, down, table, COARSE),
        scratch=[coarse_ghosts, scratch(128), scratch(128), scratch(512)],
    )
    image, sums = call(
        image_kernel, "image", [fine, f32(lax.axis_size("inner"), 1, LANES)],
        residual_in, direction, *exchange(up, down, table, FINE), scratch=[fine_ghosts],
    )
    received = lax.all_to_all(sums, "inner", 0, 0, tiled=True)
    (sums,) = call(add_kernel, "add", [f32(lax.axis_size("outer"), 1, LANES)], received)
    received = lax.all_to_all(sums, "outer", 0, 0, tiled=True)
    solved, left, norm = call(
        finish_kernel, "finish", [fine, fine, f32(8, LANES)], received, residual_in, direction, image
    )
    return solved, left, norm[0, 0]


def solution(mesh):
    devices = mesh.devices.reshape(-1, GROUP)
    split = Mesh(devices, AXES)
    return jax.shard_map(
        local,
        mesh=split,
        in_specs=(P(None, AXES), P(), P(None, AXES)),
        out_specs=(P(None, AXES), P(None, AXES), P()),
        check_vma=False,
    )
```

```python
import functools

import jax
import jax.numpy as jnp
from jax import lax
from jax.experimental import pallas as pl
from jax.experimental.pallas import tpu as pltpu
from jax.sharding import Mesh
from jax.sharding import PartitionSpec as P

LANES = 128
TAIL = 64
FINE = 192
COARSE = 48
GROUP = 16
GRANT = 8 * 1024 * 1024
AXES = ("outer", "inner")
RELAX_FINE = (2.0 / 3.0) / 6.0
RELAX_COARSE = (2.0 / 3.0) / 1.5

VMEM = pl.BlockSpec(memory_space=pltpu.VMEM)
SMEM = pl.BlockSpec(memory_space=pltpu.SMEM)

LANE_ROW = 0
WINDOW_ROW = 8
FORWARD_UP = 16
FORWARD_DOWN = 24
UPPER_NEAR = 32
UPPER_FAR = 40
TABLE_ROWS = 48


def f32(*shape):
    return jax.ShapeDtypeStruct(shape, jnp.float32)


def i32(*shape):
    return jax.ShapeDtypeStruct(shape, jnp.int32)


def call(kernel, name, outs, *args, in_specs=None, out_specs=None, scratch=()):
    return pl.pallas_call(
        kernel,
        out_shape=outs,
        in_specs=in_specs or [VMEM] * len(args),
        out_specs=out_specs or [VMEM] * len(outs),
        scratch_shapes=list(scratch),
        compiler_params=pltpu.CompilerParams(vmem_limit_bytes=GRANT),
        name=name,
    )(*args)


def take(block, lanes):
    return jnp.take_along_axis(block, lanes, axis=1, mode="promise_in_bounds")


class Chosen:
    def __init__(self, flag, if_set, if_clear):
        self.flag, self.if_set, self.if_clear = flag, if_set, if_clear

    def __getitem__(self, at):
        return jnp.where(self.flag, self.if_set[at], self.if_clear[at])


def write_pair(table, flag_row, up, down, inner, outer, rows):
    upper = table[flag_row : flag_row + 8, :] > 0
    for row in range(0, rows, 8):
        high = up[row : row + 8, :]
        low = down[row : row + 8, :]
        inner[row : row + 8, :] = jnp.where(upper, low, high)
        outer[row : row + 8, :] = jnp.where(upper, high, low)


def write_faces(values, up, down):
    up[0:64, :] = values[448:512, :]
    down[0:64, :] = values[0:64, :]
    for x in range(8):
        up[64 + 8 * x : 72 + 8 * x, :] = values[64 * x + 56 : 64 * x + 64, :]
        down[64 + 8 * x : 72 + 8 * x, :] = values[64 * x : 64 * x + 8, :]
    up[128:192, :] = values[pl.ds(7, 64, stride=8), :]
    down[128:192, :] = values[pl.ds(0, 64, stride=8), :]


def write_coarse_faces(values, up, down):
    up[0:16, :] = values[48:64, :]
    down[0:16, :] = values[0:16, :]
    for x in range(4):
        up[16 + 4 * x : 20 + 4 * x, :] = values[16 * x + 12 : 16 * x + 16, :]
        down[16 + 4 * x : 20 + 4 * x, :] = values[16 * x : 16 * x + 4, :]
    up[32:48, :] = values[pl.ds(3, 16, stride=4), :]
    down[32:48, :] = values[pl.ds(0, 16, stride=4), :]


def windows_of(table, up, down, near_inner, near_outer, far_inner, far_outer):
    near = table[UPPER_NEAR : UPPER_NEAR + 8, :] > 0
    far = table[UPPER_FAR : UPPER_FAR + 8, :] > 0
    return (
        (up, Chosen(near, near_inner, near_outer), Chosen(far, far_inner, far_outer)),
        (down, Chosen(near, near_outer, near_inner), Chosen(far, far_outer, far_inner)),
    )


def read_ghosts(table, faces, ghosts, rows):
    windows = windows_of(table, *faces)
    per_face = rows // 3
    packed = rows // 2
    for face in range(6):
        own, near, far = windows[face % 2]
        lane = jnp.broadcast_to(table[LANE_ROW + face : LANE_ROW + face + 1, :], (8, LANES))
        window = jnp.broadcast_to(table[WINDOW_ROW + face : WINDOW_ROW + face + 1, :], (8, LANES))
        is_own, is_near, is_far, is_last = [window == which for which in range(4)]
        first_half = jnp.minimum(lane, TAIL - 1)
        second_half = first_half + TAIL
        for step in range(0, per_face, 8):
            row = (face // 2) * per_face + step
            last_row = rows + row % packed
            last_lane = first_half if row < packed else second_half
            picked = jnp.where(is_last, take(far[last_row : last_row + 8, :], last_lane), 0.0)
            picked = jnp.where(is_far, take(far[row : row + 8, :], lane), picked)
            picked = jnp.where(is_near, take(near[row : row + 8, :], lane), picked)
            picked = jnp.where(is_own, take(own[row : row + 8, :], lane), picked)
            ghosts[face * per_face + step : face * per_face + step + 8, :] = picked


def beside(values, ghosts, x, y):
    sub = lax.broadcasted_iota(jnp.int32, (8, LANES), 0)
    at = 64 * x + 8 * y
    line = 8 * x + y
    centre = values[at : at + 8, :]
    below_x = values[at - 64 : at - 56, :] if x > 0 else ghosts[8 * y : 8 * y + 8, :]
    above_x = values[at + 64 : at + 72, :] if x < 7 else ghosts[64 + 8 * y : 72 + 8 * y, :]
    below_y = values[at - 8 : at, :] if y > 0 else ghosts[128 + 8 * x : 136 + 8 * x, :]
    above_y = values[at + 8 : at + 16, :] if y < 7 else ghosts[192 + 8 * x : 200 + 8 * x, :]
    below_z = jnp.where(sub == 0, ghosts[256 + line : 257 + line, :], pltpu.roll(centre, 1, 0))
    above_z = jnp.where(sub == 7, ghosts[320 + line : 321 + line, :], pltpu.roll(centre, 7, 0))
    return centre, ((above_x + below_x) + (above_y + below_y)) + (above_z + below_z)


def start_kernel(device_ref, counts_ref, right_ref, neighbours_ref, residual, up, down, inner, outer, table):
    device = device_ref[0]
    own_count = counts_ref[device]
    lane = lax.broadcasted_iota(jnp.int32, (8, LANES), 1)
    live = lane < own_count
    for row in range(0, 512, 8):
        residual[row : row + 8, :] = jnp.where(live, right_ref[row : row + 8, :], 0.0)
    write_faces(residual, up, down)
    table[UPPER_NEAR : UPPER_NEAR + 8, :] = jnp.full((8, LANES), device & 1, jnp.int32)
    table[UPPER_FAR : UPPER_FAR + 8, :] = jnp.full((8, LANES), device & 2, jnp.int32)
    write_pair(table, UPPER_NEAR, up, down, inner, outer, FINE)
    slot = neighbours_ref[...]
    present = slot >= 0
    slot = jnp.where(present, slot, 0)
    distance = jnp.abs(lax.shift_right_logical(slot, 7) - device)
    offset = slot & (LANES - 1)
    face = lax.broadcasted_iota(jnp.int32, (6, LANES), 0)
    skipped = jnp.maximum(counts_ref[jnp.maximum(device - 3, 0)] - TAIL, 0)
    shifted = jnp.where((distance == 3) & (face % 2 == 0), offset - skipped, offset)
    table[LANE_ROW : LANE_ROW + 6, :] = jnp.clip(shifted, 0, LANES - 1)
    table[WINDOW_ROW : WINDOW_ROW + 6, :] = jnp.where(present, distance, -1)
    forward = jnp.maximum(counts_ref[jnp.maximum(device - 1, 0)] - TAIL, 0)
    table[FORWARD_UP : FORWARD_UP + 8, :] = (lane & (TAIL - 1)) + forward
    table[FORWARD_DOWN : FORWARD_DOWN + 8, :] = lane & (TAIL - 1)


def pack_kernel(rows, up, down, near_inner, near_outer, table, inner, outer):
    half = rows // 2
    lane = lax.broadcasted_iota(jnp.int32, (8, LANES), 1)
    write_pair(table, UPPER_FAR, up, down, inner, outer, rows)
    near = table[UPPER_NEAR : UPPER_NEAR + 8, :] > 0
    upper = table[UPPER_FAR : UPPER_FAR + 8, :] > 0
    near_up = Chosen(near, near_inner, near_outer)
    near_down = Chosen(near, near_outer, near_inner)

    def packed(block, lanes, row):
        first = take(block[row : row + 8, :], lanes)
        second = take(block[half + row : half + row + 8, :], lanes)
        return jnp.where(lane < TAIL, first, second)

    lanes_up = table[FORWARD_UP : FORWARD_UP + 8, :]
    lanes_down = table[FORWARD_DOWN : FORWARD_DOWN + 8, :]
    for row in range(0, half, 8):
        high = packed(near_up, lanes_up, row)
        low = packed(near_down, lanes_down, row)
        inner[rows + row : rows + row + 8, :] = jnp.where(upper, low, high)
        outer[rows + row : rows + row + 8, :] = jnp.where(upper, high, low)


def smooth_kernel(residual, *refs):
    *faces, table, out, out_up, out_down, out_inner, out_outer, ghosts = refs
    read_ghosts(table, faces, ghosts, FINE)
    for x in range(8):
        for y in range(8):
            centre, around = beside(residual, ghosts, x, y)
            first = RELAX_FINE * centre
            applied = 6.0 * first - RELAX_FINE * around
            at = 64 * x + 8 * y
            out[at : at + 8, :] = first + RELAX_FINE * (centre - applied)
    write_faces(out, out_up, out_down)
    write_pair(table, UPPER_NEAR, out_up, out_down, out_inner, out_outer, FINE)


def defect_kernel(residual, second, *refs):
    *faces, table, defect, coarse, out_up, out_down, out_inner, out_outer, ghosts, sums, scaled = refs
    read_ghosts(table, faces, ghosts, FINE)
    for big_x in range(4):
        for big_y in range(4):
            total = None
            for x in (2 * big_x, 2 * big_x + 1):
                for y in (2 * big_y, 2 * big_y + 1):
                    centre, around = beside(second, ghosts, x, y)
                    at = 64 * x + 8 * y
                    part = residual[at : at + 8, :] - (6.0 * centre - around)
                    defect[at : at + 8, :] = part
                    total = part if total is None else total + part
            at = 32 * big_x + 8 * big_y
            sums[at : at + 8, :] = total
    restricted = (sums[pl.ds(0, 64, stride=2), :] + sums[pl.ds(1, 64, stride=2), :]) * 0.125
    coarse[...] = restricted
    scaled[...] = RELAX_COARSE * restricted
    write_coarse_faces(scaled, out_up, out_down)
    write_pair(table, UPPER_NEAR, out_up, out_down, out_inner, out_outer, COARSE)


def coarse_kernel(coarse, *refs):
    *faces, table, out, out_up, out_down, out_inner, out_outer, ghosts, low_y, high_y, low_z, high_z = refs
    read_ghosts(table, faces, ghosts, COARSE)
    for x in range(4):
        low_y[16 * x : 16 * x + 4, :] = ghosts[32 + 4 * x : 36 + 4 * x, :]
        high_y[16 * x + 12 : 16 * x + 16, :] = ghosts[48 + 4 * x : 52 + 4 * x, :]
    low_z[pl.ds(0, 16, stride=4), :] = ghosts[64:80, :]
    high_z[pl.ds(3, 16, stride=4), :] = ghosts[80:96, :]
    rhs = coarse[...]
    first = RELAX_COARSE * rhs
    row = lax.broadcasted_iota(jnp.int32, (64, LANES), 0)
    below_x = jnp.concatenate([ghosts[0:16, :], first[0:48, :]], axis=0)
    above_x = jnp.concatenate([first[16:64, :], ghosts[16:32, :]], axis=0)
    below_y = jnp.where((row & 15) < 4, low_y[...], pltpu.roll(first, 4, 0))
    above_y = jnp.where((row & 15) >= 12, high_y[...], pltpu.roll(first, 60, 0))
    below_z = jnp.where((row & 3) == 0, low_z[...], pltpu.roll(first, 1, 0))
    above_z = jnp.where((row & 3) == 3, high_z[...], pltpu.roll(first, 63, 0))
    around = ((above_x + below_x) + (above_y + below_y)) + (above_z + below_z)
    out[...] = first + RELAX_COARSE * (rhs - (6.0 * first - around) * 0.25)
    write_coarse_faces(out, out_up, out_down)
    write_pair(table, UPPER_NEAR, out_up, out_down, out_inner, out_outer, COARSE)


def correct_kernel(second, defect, coarse, *refs):
    *faces, table, out, out_up, out_down, out_inner, out_outer, ghosts, wide, wide_ghosts, spread = refs
    read_ghosts(table, faces, ghosts, COARSE)
    wide[pl.ds(0, 64, stride=2), :] = coarse[...]
    wide[pl.ds(1, 64, stride=2), :] = coarse[...]
    wide_ghosts[pl.ds(0, 64, stride=2), :] = ghosts[0:64, :]
    wide_ghosts[pl.ds(1, 64, stride=2), :] = ghosts[0:64, :]
    for x in range(8):
        for y in range(8):
            at = 64 * x + 8 * y
            source = 32 * (x // 2) + 8 * (y // 2)
            spread[at : at + 8, :] = wide[source : source + 8, :]
    sub = lax.broadcasted_iota(jnp.int32, (8, LANES), 0)
    for x in range(8):
        for y in range(8):
            at = 64 * x + 8 * y
            cell = 4 * (x // 2) + y // 2
            centre = spread[at : at + 8, :]
            side_x = 8 * (y // 2)
            side_y = 8 * (x // 2)
            below_x = spread[at - 64 : at - 56, :] if x > 0 else wide_ghosts[side_x : side_x + 8, :]
            above_x = spread[at + 64 : at + 72, :] if x < 7 else wide_ghosts[32 + side_x : 40 + side_x, :]
            below_y = spread[at - 8 : at, :] if y > 0 else wide_ghosts[64 + side_y : 72 + side_y, :]
            above_y = spread[at + 8 : at + 16, :] if y < 7 else wide_ghosts[96 + side_y : 104 + side_y, :]
            below_z = jnp.where(sub == 0, ghosts[64 + cell : 65 + cell, :], pltpu.roll(centre, 1, 0))
            above_z = jnp.where(sub == 7, ghosts[80 + cell : 81 + cell, :], pltpu.roll(centre, 7, 0))
            around = ((above_x + below_x) + (above_y + below_y)) + (above_z + below_z)
            left = defect[at : at + 8, :] - (6.0 * centre - around)
            out[at : at + 8, :] = (second[at : at + 8, :] + centre) + RELAX_FINE * left
    write_faces(out, out_up, out_down)
    write_pair(table, UPPER_NEAR, out_up, out_down, out_inner, out_outer, FINE)


def image_kernel(residual, direction, *refs):
    *faces, table, image, sums, ghosts = refs
    read_ghosts(table, faces, ghosts, FINE)
    zero = jnp.zeros((8, LANES), jnp.float32)
    parts = [zero] * 5
    for x in range(8):
        for y in range(8):
            centre, around = beside(direction, ghosts, x, y)
            at = 64 * x + 8 * y
            applied = 6.0 * centre - around
            image[at : at + 8, :] = applied
            start = residual[at : at + 8, :]
            terms = (start * centre, centre * applied, start * start, start * applied, applied * applied)
            parts = [part + term for part, term in zip(parts, terms)]
    lane = lax.broadcasted_iota(jnp.int32, (1, LANES), 1)
    row = jnp.zeros((1, LANES), jnp.float32)
    for index, part in enumerate(parts):
        row = jnp.where(lane == index, jnp.sum(part), row)
    for copy in range(sums.shape[0]):
        sums[copy] = row


def add_kernel(received, out):
    total = received[0]
    for index in range(1, received.shape[0]):
        total = total + received[index]
    for copy in range(out.shape[0]):
        out[copy] = total


def finish_kernel(received, residual, direction, image, solution, left, norm):
    total = received[0]
    for index in range(1, received.shape[0]):
        total = total + received[index]
    lane = lax.broadcasted_iota(jnp.int32, (1, LANES), 1)
    along, curvature, old_square, cross_term, image_square = [
        jnp.full((8, LANES), jnp.sum(jnp.where(lane == index, total, 0.0)), jnp.float32) for index in range(5)
    ]
    step_size = along / curvature
    for row in range(0, 512, 8):
        solution[row : row + 8, :] = step_size * direction[row : row + 8, :]
        left[row : row + 8, :] = residual[row : row + 8, :] - step_size * image[row : row + 8, :]
    norm[...] = jnp.sqrt(old_square - 2.0 * step_size * cross_term + step_size * step_size * image_square)


def swap(block, distance, offset):
    count = lax.axis_size(AXES)
    route = []
    for low in range(offset - 2 * distance, count):
        if low >= 0 and low + distance < count and (low - offset) % (2 * distance) < distance:
            route += [(low, low + distance), (low + distance, low)]
    return lax.ppermute(block, AXES, route)


def exchange(up, down, inner, outer, table, rows):
    near_outer = swap(outer, 1, 1)
    near_inner = swap(inner, 1, 0)
    message = f32(rows + rows // 2, LANES)
    inner, outer = call(
        functools.partial(pack_kernel, rows), "pack", [message] * 2, up, down, near_inner, near_outer, table
    )
    far_outer = swap(outer, 2, 2)
    far_inner = swap(inner, 2, 0)
    return up, down, near_inner, near_outer, far_inner, far_outer, table


def local(right_side, counts, neighbours):
    device = lax.axis_index(AXES).astype(jnp.int32).reshape(1)
    fine = f32(512, LANES)
    faces = [f32(FINE, LANES)] * 4
    coarse = f32(64, LANES)
    coarse_faces = [f32(COARSE, LANES)] * 4
    fine_ghosts = pltpu.VMEM((2 * FINE, LANES), jnp.float32)
    coarse_ghosts = pltpu.VMEM((2 * COARSE, LANES), jnp.float32)
    scratch = lambda rows: pltpu.VMEM((rows, LANES), jnp.float32)

    residual_in, *sides, table = call(
        start_kernel, "start", [fine, *faces, i32(TABLE_ROWS, LANES)], device, counts, right_side, neighbours,
        in_specs=[SMEM, SMEM, VMEM, VMEM],
    )
    second, *sides = call(
        smooth_kernel, "smooth", [fine, *faces], residual_in, *exchange(*sides, table, FINE), scratch=[fine_ghosts]
    )
    defect, rhs, *sides = call(
        defect_kernel, "defect", [fine, coarse, *coarse_faces],
        residual_in, second, *exchange(*sides, table, FINE), scratch=[fine_ghosts, scratch(128), scratch(64)],
    )
    correction, *sides = call(
        coarse_kernel, "coarse", [coarse, *coarse_faces],
        rhs, *exchange(*sides, table, COARSE), scratch=[coarse_ghosts] + [scratch(64)] * 4,
    )
    direction, *sides = call(
        correct_kernel, "correct", [fine, *faces],
        second, defect, correction, *exchange(*sides, table, COARSE),
        scratch=[coarse_ghosts, scratch(128), scratch(128), scratch(512)],
    )
    image, sums = call(
        image_kernel, "image", [fine, f32(lax.axis_size("inner"), 1, LANES)],
        residual_in, direction, *exchange(*sides, table, FINE), scratch=[fine_ghosts],
    )
    received = lax.all_to_all(sums, "inner", 0, 0, tiled=True)
    (sums,) = call(add_kernel, "add", [f32(lax.axis_size("outer"), 1, LANES)], received)
    received = lax.all_to_all(sums, "outer", 0, 0, tiled=True)
    solved, left, norm = call(
        finish_kernel, "finish", [fine, fine, f32(8, LANES)], received, residual_in, direction, image
    )
    return solved, left, norm[0, 0]


def solution(mesh):
    devices = mesh.devices.reshape(-1, GROUP)
    split = Mesh(devices, AXES)
    return jax.shard_map(
        local,
        mesh=split,
        in_specs=(P(None, AXES), P(), P(None, AXES)),
        out_specs=(P(None, AXES), P(None, AXES), P()),
        check_vma=False,
    )
```

```python
import functools

import jax
import jax.numpy as jnp
from jax import lax
from jax.experimental import pallas as pl
from jax.experimental.pallas import tpu as pltpu
from jax.sharding import Mesh
from jax.sharding import PartitionSpec as P


LANES = 128
TAIL = 64
FINE = 192
COARSE = 48
GROUP = 16
GRANT = 8 * 1024 * 1024
AXES = ("outer", "inner")
RELAX_FINE = (2.0 / 3.0) / 6.0
RELAX_COARSE = (2.0 / 3.0) / 1.5

VMEM = pl.BlockSpec(memory_space=pltpu.VMEM)
SMEM = pl.BlockSpec(memory_space=pltpu.SMEM)

LANE_ROW = 0
WINDOW_ROW = 8
FORWARD_UP = 16
FORWARD_DOWN = 24
UPPER_NEAR = 32
UPPER_FAR = 40
TABLE_ROWS = 48


def f32(*shape):
    return jax.ShapeDtypeStruct(shape, jnp.float32)


def i32(*shape):
    return jax.ShapeDtypeStruct(shape, jnp.int32)


def call(kernel, outs, *args, in_specs=None, out_specs=None, scratch=()):
    return pl.pallas_call(
        kernel,
        out_shape=outs,
        in_specs=in_specs or [VMEM] * len(args),
        out_specs=out_specs or [VMEM] * len(outs),
        scratch_shapes=list(scratch),
        compiler_params=pltpu.CompilerParams(vmem_limit_bytes=GRANT),
    )(*args)


def take(block, lanes):
    return jnp.take_along_axis(block, lanes, axis=1, mode="promise_in_bounds")


class Chosen:
    def __init__(self, flag, if_set, if_clear):
        self.flag, self.if_set, self.if_clear = flag, if_set, if_clear

    def __getitem__(self, at):
        return jnp.where(self.flag, self.if_set[at], self.if_clear[at])


def write_pair(table, flag_row, up, down, inner, outer, rows):
    upper = table[flag_row : flag_row + 8, :] > 0
    for row in range(0, rows, 8):
        high = up[row : row + 8, :]
        low = down[row : row + 8, :]
        inner[row : row + 8, :] = jnp.where(upper, low, high)
        outer[row : row + 8, :] = jnp.where(upper, high, low)


def write_faces(values, up, down):
    up[0:64, :] = values[448:512, :]
    down[0:64, :] = values[0:64, :]
    for x in range(8):
        up[64 + 8 * x : 72 + 8 * x, :] = values[64 * x + 56 : 64 * x + 64, :]
        down[64 + 8 * x : 72 + 8 * x, :] = values[64 * x : 64 * x + 8, :]
    up[128:192, :] = values[pl.ds(7, 64, stride=8), :]
    down[128:192, :] = values[pl.ds(0, 64, stride=8), :]


def write_coarse_faces(values, up, down):
    up[0:16, :] = values[48:64, :]
    down[0:16, :] = values[0:16, :]
    for x in range(4):
        up[16 + 4 * x : 20 + 4 * x, :] = values[16 * x + 12 : 16 * x + 16, :]
        down[16 + 4 * x : 20 + 4 * x, :] = values[16 * x : 16 * x + 4, :]
    up[32:48, :] = values[pl.ds(3, 16, stride=4), :]
    down[32:48, :] = values[pl.ds(0, 16, stride=4), :]


def windows_of(table, up, down, near_inner, near_outer, far_inner, far_outer):
    near = table[UPPER_NEAR : UPPER_NEAR + 8, :] > 0
    far = table[UPPER_FAR : UPPER_FAR + 8, :] > 0
    return (
        (up, Chosen(near, near_inner, near_outer), Chosen(far, far_inner, far_outer)),
        (down, Chosen(near, near_outer, near_inner), Chosen(far, far_outer, far_inner)),
    )


def read_ghosts(table, faces, ghosts, rows):
    windows = windows_of(table, *faces)
    per_face = rows // 3
    packed = rows // 2
    for face in range(6):
        own, near, far = windows[face % 2]
        lane = jnp.broadcast_to(table[LANE_ROW + face : LANE_ROW + face + 1, :], (8, LANES))
        window = jnp.broadcast_to(table[WINDOW_ROW + face : WINDOW_ROW + face + 1, :], (8, LANES))
        is_own, is_near, is_far, is_last = [window == which for which in range(4)]
        first_half = jnp.minimum(lane, TAIL - 1)
        second_half = first_half + TAIL
        for step in range(0, per_face, 8):
            row = (face // 2) * per_face + step
            last_row = rows + row % packed
            last_lane = first_half if row < packed else second_half
            picked = jnp.where(is_last, take(far[last_row : last_row + 8, :], last_lane), 0.0)
            picked = jnp.where(is_far, take(far[row : row + 8, :], lane), picked)
            picked = jnp.where(is_near, take(near[row : row + 8, :], lane), picked)
            picked = jnp.where(is_own, take(own[row : row + 8, :], lane), picked)
            ghosts[face * per_face + step : face * per_face + step + 8, :] = picked


def beside(values, ghosts, x, y):
    sub = lax.broadcasted_iota(jnp.int32, (8, LANES), 0)
    at = 64 * x + 8 * y
    line = 8 * x + y
    centre = values[at : at + 8, :]
    below_x = values[at - 64 : at - 56, :] if x > 0 else ghosts[8 * y : 8 * y + 8, :]
    above_x = values[at + 64 : at + 72, :] if x < 7 else ghosts[64 + 8 * y : 72 + 8 * y, :]
    below_y = values[at - 8 : at, :] if y > 0 else ghosts[128 + 8 * x : 136 + 8 * x, :]
    above_y = values[at + 8 : at + 16, :] if y < 7 else ghosts[192 + 8 * x : 200 + 8 * x, :]
    below_z = jnp.where(sub == 0, ghosts[256 + line : 257 + line, :], pltpu.roll(centre, 1, 0))
    above_z = jnp.where(sub == 7, ghosts[320 + line : 321 + line, :], pltpu.roll(centre, 7, 0))
    return centre, ((above_x + below_x) + (above_y + below_y)) + (above_z + below_z)


def start_kernel(device_ref, counts_ref, right_ref, neighbours_ref, residual, up, down, inner, outer, table):
    device = device_ref[0]
    own_count = counts_ref[device]
    lane = lax.broadcasted_iota(jnp.int32, (8, LANES), 1)
    live = lane < own_count
    for row in range(0, 512, 8):
        residual[row : row + 8, :] = jnp.where(live, right_ref[row : row + 8, :], 0.0)
    write_faces(residual, up, down)
    table[UPPER_NEAR : UPPER_NEAR + 8, :] = jnp.full((8, LANES), device & 1, jnp.int32)
    table[UPPER_FAR : UPPER_FAR + 8, :] = jnp.full((8, LANES), device & 2, jnp.int32)
    write_pair(table, UPPER_NEAR, up, down, inner, outer, FINE)
    slot = neighbours_ref[...]
    present = slot >= 0
    slot = jnp.where(present, slot, 0)
    distance = jnp.abs(lax.shift_right_logical(slot, 7) - device)
    offset = slot & (LANES - 1)
    face = lax.broadcasted_iota(jnp.int32, (6, LANES), 0)
    skipped = jnp.maximum(counts_ref[jnp.maximum(device - 3, 0)] - TAIL, 0)
    shifted = jnp.where((distance == 3) & (face % 2 == 0), offset - skipped, offset)
    table[LANE_ROW : LANE_ROW + 6, :] = jnp.clip(shifted, 0, LANES - 1)
    table[WINDOW_ROW : WINDOW_ROW + 6, :] = jnp.where(present, distance, -1)
    forward = jnp.maximum(counts_ref[jnp.maximum(device - 1, 0)] - TAIL, 0)
    table[FORWARD_UP : FORWARD_UP + 8, :] = (lane & (TAIL - 1)) + forward
    table[FORWARD_DOWN : FORWARD_DOWN + 8, :] = lane & (TAIL - 1)


def pack_kernel(rows, up, down, near_inner, near_outer, table, inner, outer):
    half = rows // 2
    lane = lax.broadcasted_iota(jnp.int32, (8, LANES), 1)
    write_pair(table, UPPER_FAR, up, down, inner, outer, rows)
    near = table[UPPER_NEAR : UPPER_NEAR + 8, :] > 0
    upper = table[UPPER_FAR : UPPER_FAR + 8, :] > 0
    near_up = Chosen(near, near_inner, near_outer)
    near_down = Chosen(near, near_outer, near_inner)

    def packed(block, lanes, row):
        first = take(block[row : row + 8, :], lanes)
        second = take(block[half + row : half + row + 8, :], lanes)
        return jnp.where(lane < TAIL, first, second)

    lanes_up = table[FORWARD_UP : FORWARD_UP + 8, :]
    lanes_down = table[FORWARD_DOWN : FORWARD_DOWN + 8, :]
    for row in range(0, half, 8):
        high = packed(near_up, lanes_up, row)
        low = packed(near_down, lanes_down, row)
        inner[rows + row : rows + row + 8, :] = jnp.where(upper, low, high)
        outer[rows + row : rows + row + 8, :] = jnp.where(upper, high, low)


def smooth_kernel(residual, *refs):
    *faces, table, out, out_up, out_down, out_inner, out_outer, ghosts = refs
    read_ghosts(table, faces, ghosts, FINE)
    for x in range(8):
        for y in range(8):
            centre, around = beside(residual, ghosts, x, y)
            first = RELAX_FINE * centre
            applied = 6.0 * first - RELAX_FINE * around
            at = 64 * x + 8 * y
            out[at : at + 8, :] = first + RELAX_FINE * (centre - applied)
    write_faces(out, out_up, out_down)
    write_pair(table, UPPER_NEAR, out_up, out_down, out_inner, out_outer, FINE)


def defect_kernel(residual, second, *refs):
    *faces, table, defect, coarse, out_up, out_down, out_inner, out_outer, ghosts, sums, scaled = refs
    read_ghosts(table, faces, ghosts, FINE)
    for big_x in range(4):
        for big_y in range(4):
            total = None
            for x in (2 * big_x, 2 * big_x + 1):
                for y in (2 * big_y, 2 * big_y + 1):
                    centre, around = beside(second, ghosts, x, y)
                    at = 64 * x + 8 * y
                    part = residual[at : at + 8, :] - (6.0 * centre - around)
                    defect[at : at + 8, :] = part
                    total = part if total is None else total + part
            at = 32 * big_x + 8 * big_y
            sums[at : at + 8, :] = total
    restricted = (sums[pl.ds(0, 64, stride=2), :] + sums[pl.ds(1, 64, stride=2), :]) * 0.125
    coarse[...] = restricted
    scaled[...] = RELAX_COARSE * restricted
    write_coarse_faces(scaled, out_up, out_down)
    write_pair(table, UPPER_NEAR, out_up, out_down, out_inner, out_outer, COARSE)


def coarse_kernel(coarse, *refs):
    *faces, table, out, out_up, out_down, out_inner, out_outer, ghosts, low_y, high_y, low_z, high_z = refs
    read_ghosts(table, faces, ghosts, COARSE)
    for x in range(4):
        low_y[16 * x : 16 * x + 4, :] = ghosts[32 + 4 * x : 36 + 4 * x, :]
        high_y[16 * x + 12 : 16 * x + 16, :] = ghosts[48 + 4 * x : 52 + 4 * x, :]
    low_z[pl.ds(0, 16, stride=4), :] = ghosts[64:80, :]
    high_z[pl.ds(3, 16, stride=4), :] = ghosts[80:96, :]
    rhs = coarse[...]
    first = RELAX_COARSE * rhs
    row = lax.broadcasted_iota(jnp.int32, (64, LANES), 0)
    below_x = jnp.concatenate([ghosts[0:16, :], first[0:48, :]], axis=0)
    above_x = jnp.concatenate([first[16:64, :], ghosts[16:32, :]], axis=0)
    below_y = jnp.where((row & 15) < 4, low_y[...], pltpu.roll(first, 4, 0))
    above_y = jnp.where((row & 15) >= 12, high_y[...], pltpu.roll(first, 60, 0))
    below_z = jnp.where((row & 3) == 0, low_z[...], pltpu.roll(first, 1, 0))
    above_z = jnp.where((row & 3) == 3, high_z[...], pltpu.roll(first, 63, 0))
    around = ((above_x + below_x) + (above_y + below_y)) + (above_z + below_z)
    out[...] = first + RELAX_COARSE * (rhs - (6.0 * first - around) * 0.25)
    write_coarse_faces(out, out_up, out_down)
    write_pair(table, UPPER_NEAR, out_up, out_down, out_inner, out_outer, COARSE)


def correct_kernel(second, defect, coarse, *refs):
    *faces, table, out, out_up, out_down, out_inner, out_outer, ghosts, wide, wide_ghosts, spread = refs
    read_ghosts(table, faces, ghosts, COARSE)
    wide[pl.ds(0, 64, stride=2), :] = coarse[...]
    wide[pl.ds(1, 64, stride=2), :] = coarse[...]
    wide_ghosts[pl.ds(0, 64, stride=2), :] = ghosts[0:64, :]
    wide_ghosts[pl.ds(1, 64, stride=2), :] = ghosts[0:64, :]
    for x in range(8):
        for y in range(8):
            at = 64 * x + 8 * y
            source = 32 * (x // 2) + 8 * (y // 2)
            spread[at : at + 8, :] = wide[source : source + 8, :]
    sub = lax.broadcasted_iota(jnp.int32, (8, LANES), 0)
    for x in range(8):
        for y in range(8):
            at = 64 * x + 8 * y
            cell = 4 * (x // 2) + y // 2
            centre = spread[at : at + 8, :]
            side_x = 8 * (y // 2)
            side_y = 8 * (x // 2)
            below_x = spread[at - 64 : at - 56, :] if x > 0 else wide_ghosts[side_x : side_x + 8, :]
            above_x = spread[at + 64 : at + 72, :] if x < 7 else wide_ghosts[32 + side_x : 40 + side_x, :]
            below_y = spread[at - 8 : at, :] if y > 0 else wide_ghosts[64 + side_y : 72 + side_y, :]
            above_y = spread[at + 8 : at + 16, :] if y < 7 else wide_ghosts[96 + side_y : 104 + side_y, :]
            below_z = jnp.where(sub == 0, ghosts[64 + cell : 65 + cell, :], pltpu.roll(centre, 1, 0))
            above_z = jnp.where(sub == 7, ghosts[80 + cell : 81 + cell, :], pltpu.roll(centre, 7, 0))
            around = ((above_x + below_x) + (above_y + below_y)) + (above_z + below_z)
            left = defect[at : at + 8, :] - (6.0 * centre - around)
            out[at : at + 8, :] = (second[at : at + 8, :] + centre) + RELAX_FINE * left
    write_faces(out, out_up, out_down)
    write_pair(table, UPPER_NEAR, out_up, out_down, out_inner, out_outer, FINE)


def image_kernel(residual, direction, *refs):
    *faces, table, image, sums, ghosts = refs
    read_ghosts(table, faces, ghosts, FINE)
    zero = jnp.zeros((8, LANES), jnp.float32)
    parts = [zero] * 5
    for x in range(8):
        for y in range(8):
            centre, around = beside(direction, ghosts, x, y)
            at = 64 * x + 8 * y
            applied = 6.0 * centre - around
            image[at : at + 8, :] = applied
            start = residual[at : at + 8, :]
            terms = (start * centre, centre * applied, start * start, start * applied, applied * applied)
            parts = [part + term for part, term in zip(parts, terms)]
    lane = lax.broadcasted_iota(jnp.int32, (1, LANES), 1)
    row = jnp.zeros((1, LANES), jnp.float32)
    for index, part in enumerate(parts):
        row = jnp.where(lane == index, jnp.sum(part), row)
    for copy in range(sums.shape[0]):
        sums[copy] = row


def add_kernel(received, out):
    total = received[0]
    for index in range(1, received.shape[0]):
        total = total + received[index]
    for copy in range(out.shape[0]):
        out[copy] = total


def finish_kernel(received, residual, direction, image, solution, left, norm):
    total = received[0]
    for index in range(1, received.shape[0]):
        total = total + received[index]
    lane = lax.broadcasted_iota(jnp.int32, (1, LANES), 1)
    along, curvature, old_square, cross_term, image_square = [
        jnp.full((8, LANES), jnp.sum(jnp.where(lane == index, total, 0.0)), jnp.float32) for index in range(5)
    ]
    step_size = along / curvature
    for row in range(0, 512, 8):
        solution[row : row + 8, :] = step_size * direction[row : row + 8, :]
        left[row : row + 8, :] = residual[row : row + 8, :] - step_size * image[row : row + 8, :]
    norm[...] = jnp.sqrt(old_square - 2.0 * step_size * cross_term + step_size * step_size * image_square)


def swap(block, distance, offset):
    count = lax.axis_size(AXES)
    route = []
    for low in range(offset - 2 * distance, count):
        if low >= 0 and low + distance < count and (low - offset) % (2 * distance) < distance:
            route += [(low, low + distance), (low + distance, low)]
    return lax.ppermute(block, AXES, route)


def exchange(rows, up, down, inner, outer, table):
    near_outer = swap(outer, 1, 1)
    near_inner = swap(inner, 1, 0)
    message = f32(rows + rows // 2, LANES)
    inner, outer = call(functools.partial(pack_kernel, rows), [message] * 2, up, down, near_inner, near_outer, table)
    far_outer = swap(outer, 2, 2)
    far_inner = swap(inner, 2, 0)
    return up, down, near_inner, near_outer, far_inner, far_outer, table


def step(right_side, counts, neighbours):
    device = lax.axis_index(AXES).astype(jnp.int32).reshape(1)
    fine = f32(512, LANES)
    faces = [f32(FINE, LANES)] * 4
    coarse = f32(64, LANES)
    coarse_faces = [f32(COARSE, LANES)] * 4
    fine_ghosts = pltpu.VMEM((2 * FINE, LANES), jnp.float32)
    coarse_ghosts = pltpu.VMEM((2 * COARSE, LANES), jnp.float32)
    scratch = lambda rows: pltpu.VMEM((rows, LANES), jnp.float32)

    residual_in, *sides, table = call(
        start_kernel, [fine, *faces, i32(TABLE_ROWS, LANES)], device, counts, right_side, neighbours,
        in_specs=[SMEM, SMEM, VMEM, VMEM],
    )
    second, *sides = call(
        smooth_kernel, [fine, *faces], residual_in, *exchange(FINE, *sides, table), scratch=[fine_ghosts]
    )
    defect, rhs, *sides = call(
        defect_kernel, [fine, coarse, *coarse_faces],
        residual_in, second, *exchange(FINE, *sides, table), scratch=[fine_ghosts, scratch(128), scratch(64)],
    )
    correction, *sides = call(
        coarse_kernel, [coarse, *coarse_faces],
        rhs, *exchange(COARSE, *sides, table), scratch=[coarse_ghosts] + [scratch(64)] * 4,
    )
    direction, *sides = call(
        correct_kernel, [fine, *faces],
        second, defect, correction, *exchange(COARSE, *sides, table),
        scratch=[coarse_ghosts, scratch(128), scratch(128), scratch(512)],
    )
    image, sums = call(
        image_kernel, [fine, f32(lax.axis_size("inner"), 1, LANES)],
        residual_in, direction, *exchange(FINE, *sides, table), scratch=[fine_ghosts],
    )
    received = lax.all_to_all(sums, "inner", 0, 0, tiled=True)
    (sums,) = call(add_kernel, [f32(lax.axis_size("outer"), 1, LANES)], received)
    received = lax.all_to_all(sums, "outer", 0, 0, tiled=True)
    solved, left, norm = call(finish_kernel, [fine, fine, f32(8, LANES)], received, residual_in, direction, image)
    return solved, left, norm[0, 0]


def solution(mesh):
    devices = mesh.devices.reshape(-1, GROUP)
    split = Mesh(devices, AXES)
    return jax.shard_map(
        step,
        mesh=split,
        in_specs=(P(None, AXES), P(), P(None, AXES)),
        out_specs=(P(None, AXES), P(None, AXES), P()),
        check_vma=False,
    )
```

```python
import functools

import jax
import jax.numpy as jnp
from jax import lax
from jax.experimental import pallas as pl
from jax.experimental.pallas import tpu as pltpu
from jax.sharding import Mesh
from jax.sharding import PartitionSpec as P


LANES = 128
TAIL = 64
FINE = 192
PAIR = 2
BLOCK = 72
REACH = 3
GRANT = 8 * 1024 * 1024
AXES = ("outer", "pair", "row")
RELAX_FINE = (2.0 / 3.0) / 6.0
RELAX_COARSE = (2.0 / 3.0) / 1.5

VMEM = pl.BlockSpec(memory_space=pltpu.VMEM)
SMEM = pl.BlockSpec(memory_space=pltpu.SMEM)

LANE_ROW = 0
WINDOW_ROW = 8
FORWARD_UP = 16
FORWARD_DOWN = 24
UPPER_NEAR = 32
UPPER_FAR = 40
NEIGHBOUR_ROW = 48
TABLE_ROWS = 56


def f32(*shape):
    return jax.ShapeDtypeStruct(shape, jnp.float32)


def i32(*shape):
    return jax.ShapeDtypeStruct(shape, jnp.int32)


def call(kernel, outs, *args, in_specs=None, out_specs=None, scratch=()):
    return pl.pallas_call(
        kernel,
        out_shape=outs,
        in_specs=in_specs or [VMEM] * len(args),
        out_specs=out_specs or [VMEM] * len(outs),
        scratch_shapes=list(scratch),
        compiler_params=pltpu.CompilerParams(vmem_limit_bytes=GRANT),
    )(*args)


def take(block, lanes):
    return jnp.take_along_axis(block, lanes, axis=1, mode="promise_in_bounds")


class Chosen:
    def __init__(self, flag, if_set, if_clear):
        self.flag, self.if_set, self.if_clear = flag, if_set, if_clear

    def __getitem__(self, at):
        return jnp.where(self.flag, self.if_set[at], self.if_clear[at])


def write_pair(table, flag_row, up, down, inner, outer, rows):
    upper = table[flag_row : flag_row + 8, :] > 0
    for row in range(0, rows, 8):
        high = up[row : row + 8, :]
        low = down[row : row + 8, :]
        inner[row : row + 8, :] = jnp.where(upper, low, high)
        outer[row : row + 8, :] = jnp.where(upper, high, low)


def write_faces(values, up, down):
    up[0:64, :] = values[448:512, :]
    down[0:64, :] = values[0:64, :]
    for x in range(8):
        up[64 + 8 * x : 72 + 8 * x, :] = values[64 * x + 56 : 64 * x + 64, :]
        down[64 + 8 * x : 72 + 8 * x, :] = values[64 * x : 64 * x + 8, :]
    up[128:192, :] = values[pl.ds(7, 64, stride=8), :]
    down[128:192, :] = values[pl.ds(0, 64, stride=8), :]


def write_coarse_faces(values, at, faces, to):
    faces[to : to + 16, :] = values[at : at + 16, :]
    faces[to + 16 : to + 32, :] = values[at + 48 : at + 64, :]
    for x in range(4):
        faces[to + 32 + 4 * x : to + 36 + 4 * x, :] = values[at + 16 * x : at + 16 * x + 4, :]
        faces[to + 48 + 4 * x : to + 52 + 4 * x, :] = values[at + 16 * x + 12 : at + 16 * x + 16, :]
    faces[to + 64 : to + 80, :] = values[pl.ds(at, 16, stride=4), :]
    faces[to + 80 : to + 96, :] = values[pl.ds(at + 3, 16, stride=4), :]


def read_coarse_ghosts(faces, block, slots, device, ghosts):
    for face in range(6):
        slot = jnp.broadcast_to(slots[face : face + 1, :], (8, LANES))
        safe = jnp.maximum(slot, 0)
        lane = safe & (LANES - 1)
        distance = jnp.where(slot >= 0, jnp.abs(lax.shift_right_logical(safe, 7) - device), -1)
        for step in (0, 8):
            picked = jnp.zeros((8, LANES), jnp.float32)
            for which in range(REACH + 1):
                source = block - which if face % 2 == 0 else block + which
                row = 96 * source + 16 * (face ^ 1) + step
                picked = jnp.where(distance == which, take(faces[row : row + 8, :], lane), picked)
            ghosts[16 * face + step : 16 * face + step + 8, :] = picked


def windows_of(table, up, down, near_inner, near_outer, far_inner, far_outer):
    near = table[UPPER_NEAR : UPPER_NEAR + 8, :] > 0
    far = table[UPPER_FAR : UPPER_FAR + 8, :] > 0
    return (
        (up, Chosen(near, near_inner, near_outer), Chosen(far, far_inner, far_outer)),
        (down, Chosen(near, near_outer, near_inner), Chosen(far, far_outer, far_inner)),
    )


def read_ghosts(table, faces, ghosts, rows):
    windows = windows_of(table, *faces)
    per_face = rows // 3
    packed = rows // 2
    for face in range(6):
        own, near, far = windows[face % 2]
        lane = jnp.broadcast_to(table[LANE_ROW + face : LANE_ROW + face + 1, :], (8, LANES))
        window = jnp.broadcast_to(table[WINDOW_ROW + face : WINDOW_ROW + face + 1, :], (8, LANES))
        is_own, is_near, is_far, is_last = [window == which for which in range(4)]
        first_half = jnp.minimum(lane, TAIL - 1)
        second_half = first_half + TAIL
        for step in range(0, per_face, 8):
            row = (face // 2) * per_face + step
            last_row = rows + row % packed
            last_lane = first_half if row < packed else second_half
            picked = jnp.where(is_last, take(far[last_row : last_row + 8, :], last_lane), 0.0)
            picked = jnp.where(is_far, take(far[row : row + 8, :], lane), picked)
            picked = jnp.where(is_near, take(near[row : row + 8, :], lane), picked)
            picked = jnp.where(is_own, take(own[row : row + 8, :], lane), picked)
            ghosts[face * per_face + step : face * per_face + step + 8, :] = picked


def beside(values, ghosts, x, y):
    sub = lax.broadcasted_iota(jnp.int32, (8, LANES), 0)
    at = 64 * x + 8 * y
    line = 8 * x + y
    centre = values[at : at + 8, :]
    below_x = values[at - 64 : at - 56, :] if x > 0 else ghosts[8 * y : 8 * y + 8, :]
    above_x = values[at + 64 : at + 72, :] if x < 7 else ghosts[64 + 8 * y : 72 + 8 * y, :]
    below_y = values[at - 8 : at, :] if y > 0 else ghosts[128 + 8 * x : 136 + 8 * x, :]
    above_y = values[at + 8 : at + 16, :] if y < 7 else ghosts[192 + 8 * x : 200 + 8 * x, :]
    below_z = jnp.where(sub == 0, ghosts[256 + line : 257 + line, :], pltpu.roll(centre, 1, 0))
    above_z = jnp.where(sub == 7, ghosts[320 + line : 321 + line, :], pltpu.roll(centre, 7, 0))
    return centre, ((above_x + below_x) + (above_y + below_y)) + (above_z + below_z)


def start_kernel(device_ref, counts_ref, right_ref, neighbours_ref, residual, up, down, inner, outer, table):
    device = device_ref[0]
    own_count = counts_ref[device]
    lane = lax.broadcasted_iota(jnp.int32, (8, LANES), 1)
    live = lane < own_count
    for row in range(0, 512, 8):
        residual[row : row + 8, :] = jnp.where(live, right_ref[row : row + 8, :], 0.0)
    write_faces(residual, up, down)
    table[UPPER_NEAR : UPPER_NEAR + 8, :] = jnp.full((8, LANES), device & 1, jnp.int32)
    table[UPPER_FAR : UPPER_FAR + 8, :] = jnp.full((8, LANES), device & 2, jnp.int32)
    write_pair(table, UPPER_NEAR, up, down, inner, outer, FINE)
    slot = neighbours_ref[...]
    present = slot >= 0
    slot = jnp.where(present, slot, 0)
    distance = jnp.abs(lax.shift_right_logical(slot, 7) - device)
    offset = slot & (LANES - 1)
    face = lax.broadcasted_iota(jnp.int32, (6, LANES), 0)
    skipped = jnp.maximum(counts_ref[jnp.maximum(device - 3, 0)] - TAIL, 0)
    shifted = jnp.where((distance == 3) & (face % 2 == 0), offset - skipped, offset)
    table[LANE_ROW : LANE_ROW + 6, :] = jnp.clip(shifted, 0, LANES - 1)
    table[WINDOW_ROW : WINDOW_ROW + 6, :] = jnp.where(present, distance, -1)
    table[NEIGHBOUR_ROW : NEIGHBOUR_ROW + 6, :] = neighbours_ref[...]
    table[NEIGHBOUR_ROW + 6 : NEIGHBOUR_ROW + 8, :] = jnp.full((2, LANES), -1, jnp.int32)
    forward = jnp.maximum(counts_ref[jnp.maximum(device - 1, 0)] - TAIL, 0)
    table[FORWARD_UP : FORWARD_UP + 8, :] = (lane & (TAIL - 1)) + forward
    table[FORWARD_DOWN : FORWARD_DOWN + 8, :] = lane & (TAIL - 1)


def pack_kernel(rows, up, down, near_inner, near_outer, table, inner, outer):
    half = rows // 2
    lane = lax.broadcasted_iota(jnp.int32, (8, LANES), 1)
    write_pair(table, UPPER_FAR, up, down, inner, outer, rows)
    near = table[UPPER_NEAR : UPPER_NEAR + 8, :] > 0
    upper = table[UPPER_FAR : UPPER_FAR + 8, :] > 0
    near_up = Chosen(near, near_inner, near_outer)
    near_down = Chosen(near, near_outer, near_inner)

    def packed(block, lanes, row):
        first = take(block[row : row + 8, :], lanes)
        second = take(block[half + row : half + row + 8, :], lanes)
        return jnp.where(lane < TAIL, first, second)

    lanes_up = table[FORWARD_UP : FORWARD_UP + 8, :]
    lanes_down = table[FORWARD_DOWN : FORWARD_DOWN + 8, :]
    for row in range(0, half, 8):
        high = packed(near_up, lanes_up, row)
        low = packed(near_down, lanes_down, row)
        inner[rows + row : rows + row + 8, :] = jnp.where(upper, low, high)
        outer[rows + row : rows + row + 8, :] = jnp.where(upper, high, low)


def smooth_kernel(residual, *refs):
    *faces, table, out, out_up, out_down, out_inner, out_outer, ghosts = refs
    read_ghosts(table, faces, ghosts, FINE)
    for x in range(8):
        for y in range(8):
            centre, around = beside(residual, ghosts, x, y)
            first = RELAX_FINE * centre
            applied = 6.0 * first - RELAX_FINE * around
            at = 64 * x + 8 * y
            out[at : at + 8, :] = first + RELAX_FINE * (centre - applied)
    write_faces(out, out_up, out_down)
    write_pair(table, UPPER_NEAR, out_up, out_down, out_inner, out_outer, FINE)


def defect_kernel(residual, second, *refs):
    *faces, table, defect, block, ghosts, sums = refs
    read_ghosts(table, faces, ghosts, FINE)
    for big_x in range(4):
        for big_y in range(4):
            total = None
            for x in (2 * big_x, 2 * big_x + 1):
                for y in (2 * big_y, 2 * big_y + 1):
                    centre, around = beside(second, ghosts, x, y)
                    at = 64 * x + 8 * y
                    part = residual[at : at + 8, :] - (6.0 * centre - around)
                    defect[at : at + 8, :] = part
                    total = part if total is None else total + part
            at = 32 * big_x + 8 * big_y
            sums[at : at + 8, :] = total
    restricted = (sums[pl.ds(0, 64, stride=2), :] + sums[pl.ds(1, 64, stride=2), :]) * 0.125
    block[0:64, :] = restricted
    block[64:72, :] = table[NEIGHBOUR_ROW : NEIGHBOUR_ROW + 8, :].astype(jnp.float32)


def spread_kernel(device_ref, own, across, beside_row, out):
    column = device_ref[0] % out.shape[0]
    odd_row = (device_ref[0] // out.shape[0]) % 2
    for target in range(out.shape[0]):
        out[target, 0:BLOCK, :] = own[...]
        from_before = jnp.where(column > target, 1, 0)
        same = jnp.full((8, LANES), jnp.where(odd_row == from_before, 1, 0), jnp.int32) > 0
        for row in range(0, BLOCK, 8):
            other = jnp.where(same, beside_row[row : row + 8, :], across[row : row + 8, :])
            out[target, BLOCK + row : BLOCK + row + 8, :] = other


def coarse_update(first, at, ghosts, low_y, high_y, low_z, high_z):
    for x in range(4):
        low_y[16 * x : 16 * x + 4, :] = ghosts[32 + 4 * x : 36 + 4 * x, :]
        high_y[16 * x + 12 : 16 * x + 16, :] = ghosts[48 + 4 * x : 52 + 4 * x, :]
    low_z[pl.ds(0, 16, stride=4), :] = ghosts[64:80, :]
    high_z[pl.ds(3, 16, stride=4), :] = ghosts[80:96, :]
    centre = first[at : at + 64, :]
    row = lax.broadcasted_iota(jnp.int32, (64, LANES), 0)
    below_x = jnp.concatenate([ghosts[0:16, :], first[at : at + 48, :]], axis=0)
    above_x = jnp.concatenate([first[at + 16 : at + 64, :], ghosts[16:32, :]], axis=0)
    below_y = jnp.where((row & 15) < 4, low_y[...], pltpu.roll(centre, 4, 0))
    above_y = jnp.where((row & 15) >= 12, high_y[...], pltpu.roll(centre, 60, 0))
    below_z = jnp.where((row & 3) == 0, low_z[...], pltpu.roll(centre, 1, 0))
    above_z = jnp.where((row & 3) == 3, high_z[...], pltpu.roll(centre, 63, 0))
    around = ((above_x + below_x) + (above_y + below_y)) + (above_z + below_z)
    return centre + (centre - RELAX_COARSE * ((6.0 * centre - around) * 0.25))


def correct_kernel(device_ref, second, defect, received, *refs):
    table, out, out_up, out_down, out_inner, out_outer, *scratch = refs
    first, first_faces, slots, coarse, coarse_faces, ghosts, low_y, high_y, low_z, high_z, *scratch = scratch
    wide, wide_ghosts, spread = scratch
    device = device_ref[0]
    row_length = received.shape[0]
    column = device % row_length
    for block in range(4 * REACH + 1):
        place = column + (block - 2 * REACH)
        in_row = (place >= 0) & (place < row_length)
        sender = lax.rem(place + row_length, row_length)
        start = jnp.where(in_row, 0, BLOCK)
        for row in range(0, 64, 8):
            at = pl.multiple_of(start + row, 8)
            first[64 * block + row : 64 * block + row + 8, :] = RELAX_COARSE * received[sender, pl.ds(at, 8), :]
        write_coarse_faces(first, 64 * block, first_faces, 96 * block)
        if REACH <= block <= 3 * REACH:
            at = pl.multiple_of(start + 64, 8)
            to = 8 * (block - REACH)
            slots[to : to + 8, :] = received[sender, pl.ds(at, 8), :].astype(jnp.int32)
    for block in range(2 * REACH + 1):
        block_slots = slots.at[8 * block : 8 * block + 8, :]
        read_coarse_ghosts(first_faces, block + REACH, block_slots, device + (block - REACH), ghosts)
        updated = coarse_update(first, 64 * (block + REACH), ghosts, low_y, high_y, low_z, high_z)
        coarse[64 * block : 64 * block + 64, :] = updated
        write_coarse_faces(coarse, 64 * block, coarse_faces, 96 * block)
    read_coarse_ghosts(coarse_faces, REACH, slots.at[8 * REACH : 8 * REACH + 8, :], device, ghosts)
    own = coarse[64 * REACH : 64 * REACH + 64, :]
    wide[pl.ds(0, 64, stride=2), :] = own
    wide[pl.ds(1, 64, stride=2), :] = own
    wide_ghosts[pl.ds(0, 64, stride=2), :] = ghosts[0:64, :]
    wide_ghosts[pl.ds(1, 64, stride=2), :] = ghosts[0:64, :]
    for x in range(8):
        for y in range(8):
            at = 64 * x + 8 * y
            source = 32 * (x // 2) + 8 * (y // 2)
            spread[at : at + 8, :] = wide[source : source + 8, :]
    sub = lax.broadcasted_iota(jnp.int32, (8, LANES), 0)
    for x in range(8):
        for y in range(8):
            at = 64 * x + 8 * y
            cell = 4 * (x // 2) + y // 2
            centre = spread[at : at + 8, :]
            side_x = 8 * (y // 2)
            side_y = 8 * (x // 2)
            below_x = spread[at - 64 : at - 56, :] if x > 0 else wide_ghosts[side_x : side_x + 8, :]
            above_x = spread[at + 64 : at + 72, :] if x < 7 else wide_ghosts[32 + side_x : 40 + side_x, :]
            below_y = spread[at - 8 : at, :] if y > 0 else wide_ghosts[64 + side_y : 72 + side_y, :]
            above_y = spread[at + 8 : at + 16, :] if y < 7 else wide_ghosts[96 + side_y : 104 + side_y, :]
            below_z = jnp.where(sub == 0, ghosts[64 + cell : 65 + cell, :], pltpu.roll(centre, 1, 0))
            above_z = jnp.where(sub == 7, ghosts[80 + cell : 81 + cell, :], pltpu.roll(centre, 7, 0))
            around = ((above_x + below_x) + (above_y + below_y)) + (above_z + below_z)
            left = defect[at : at + 8, :] - (6.0 * centre - around)
            out[at : at + 8, :] = (second[at : at + 8, :] + centre) + RELAX_FINE * left
    write_faces(out, out_up, out_down)
    write_pair(table, UPPER_NEAR, out_up, out_down, out_inner, out_outer, FINE)


def image_kernel(residual, direction, *refs):
    *faces, table, image, sums, ghosts = refs
    read_ghosts(table, faces, ghosts, FINE)
    zero = jnp.zeros((8, LANES), jnp.float32)
    parts = [zero] * 5
    for x in range(8):
        for y in range(8):
            centre, around = beside(direction, ghosts, x, y)
            at = 64 * x + 8 * y
            applied = 6.0 * centre - around
            image[at : at + 8, :] = applied
            start = residual[at : at + 8, :]
            terms = (start * centre, centre * applied, start * start, start * applied, applied * applied)
            parts = [part + term for part, term in zip(parts, terms)]
    lane = lax.broadcasted_iota(jnp.int32, (1, LANES), 1)
    row = jnp.zeros((1, LANES), jnp.float32)
    for index, part in enumerate(parts):
        row = jnp.where(lane == index, jnp.sum(part), row)
    for copy in range(sums.shape[0]):
        sums[copy] = row


def add_kernel(received, out):
    total = received[0]
    for index in range(1, received.shape[0]):
        total = total + received[index]
    for copy in range(out.shape[0]):
        out[copy] = total


def finish_kernel(received, residual, direction, image, solution, left, norm):
    total = received[0]
    for index in range(1, received.shape[0]):
        total = total + received[index]
    lane = lax.broadcasted_iota(jnp.int32, (1, LANES), 1)
    along, curvature, old_square, cross_term, image_square = [
        jnp.full((8, LANES), jnp.sum(jnp.where(lane == index, total, 0.0)), jnp.float32) for index in range(5)
    ]
    step_size = along / curvature
    for row in range(0, 512, 8):
        solution[row : row + 8, :] = step_size * direction[row : row + 8, :]
        left[row : row + 8, :] = residual[row : row + 8, :] - step_size * image[row : row + 8, :]
    norm[...] = jnp.sqrt(old_square - 2.0 * step_size * cross_term + step_size * step_size * image_square)


def swap(block, distance, offset):
    count = lax.axis_size(AXES)
    route = []
    for low in range(offset - 2 * distance, count):
        if low >= 0 and low + distance < count and (low - offset) % (2 * distance) < distance:
            route += [(low, low + distance), (low + distance, low)]
    return lax.ppermute(block, AXES, route)


def share(block, device):
    row_length = lax.axis_size("row")
    across = swap(block, row_length, row_length)
    beside_row = swap(block, row_length, 0)
    (blocks,) = call(
        spread_kernel, [f32(row_length, 2 * BLOCK, LANES)], device, block, across, beside_row,
        in_specs=[SMEM, VMEM, VMEM, VMEM],
    )
    return lax.all_to_all(blocks, "row", 0, 0, tiled=True)


def exchange(rows, up, down, inner, outer, table):
    near_outer = swap(outer, 1, 1)
    near_inner = swap(inner, 1, 0)
    message = f32(rows + rows // 2, LANES)
    inner, outer = call(functools.partial(pack_kernel, rows), [message] * 2, up, down, near_inner, near_outer, table)
    far_outer = swap(outer, 2, 2)
    far_inner = swap(inner, 2, 0)
    return up, down, near_inner, near_outer, far_inner, far_outer, table


def step(right_side, counts, neighbours):
    device = lax.axis_index(AXES).astype(jnp.int32).reshape(1)
    fine = f32(512, LANES)
    faces = [f32(FINE, LANES)] * 4
    fine_ghosts = pltpu.VMEM((2 * FINE, LANES), jnp.float32)
    scratch = lambda rows: pltpu.VMEM((rows, LANES), jnp.float32)

    residual_in, *sides, table = call(
        start_kernel, [fine, *faces, i32(TABLE_ROWS, LANES)], device, counts, right_side, neighbours,
        in_specs=[SMEM, SMEM, VMEM, VMEM],
    )
    second, *sides = call(
        smooth_kernel, [fine, *faces], residual_in, *exchange(FINE, *sides, table), scratch=[fine_ghosts]
    )
    defect, block = call(
        defect_kernel, [fine, f32(BLOCK, LANES)],
        residual_in, second, *exchange(FINE, *sides, table), scratch=[fine_ghosts, scratch(128)],
    )
    blocks = 2 * REACH + 1
    direction, *sides = call(
        correct_kernel, [fine, *faces], device, second, defect, share(block, device), table,
        in_specs=[SMEM] + [VMEM] * 4,
        scratch=[
            scratch(64 * (4 * REACH + 1)), scratch(96 * (4 * REACH + 1)), pltpu.VMEM((8 * blocks, LANES), jnp.int32),
            scratch(64 * blocks), scratch(96 * blocks), scratch(96), *[scratch(64)] * 4,
            scratch(128), scratch(128), scratch(512),
        ],
    )
    image, sums = call(
        image_kernel, [fine, f32(lax.axis_size(AXES[1:]), 1, LANES)],
        residual_in, direction, *exchange(FINE, *sides, table), scratch=[fine_ghosts],
    )
    received = lax.all_to_all(sums, AXES[1:], 0, 0, tiled=True)
    (sums,) = call(add_kernel, [f32(lax.axis_size("outer"), 1, LANES)], received)
    received = lax.all_to_all(sums, "outer", 0, 0, tiled=True)
    solved, left, norm = call(finish_kernel, [fine, fine, f32(8, LANES)], received, residual_in, direction, image)
    return solved, left, norm[0, 0]


def solution(mesh):
    devices = mesh.devices.reshape(-1, PAIR, mesh.shape["level"])
    split = Mesh(devices, AXES)
    return jax.shard_map(
        step,
        mesh=split,
        in_specs=(P(None, AXES), P(), P(None, AXES)),
        out_specs=(P(None, AXES), P(None, AXES), P()),
        check_vma=False,
    )
```

```python
import functools

import jax
import jax.numpy as jnp
from jax import lax
from jax.experimental import pallas as pl
from jax.experimental.pallas import tpu as pltpu
from jax.sharding import Mesh
from jax.sharding import PartitionSpec as P


LANES = 128
TAIL = 64
FINE = 192
PAIR = 2
BLOCK = 72
REACH = 3
GRANT = 8 * 1024 * 1024
AXES = ("outer", "pair", "row")
RELAX_FINE = (2.0 / 3.0) / 6.0
RELAX_COARSE = (2.0 / 3.0) / 1.5

VMEM = pl.BlockSpec(memory_space=pltpu.VMEM)
SMEM = pl.BlockSpec(memory_space=pltpu.SMEM)

LANE_ROW = 0
WINDOW_ROW = 8
FORWARD_UP = 16
FORWARD_DOWN = 24
UPPER_NEAR = 32
UPPER_FAR = 40
NEIGHBOUR_ROW = 48
CROSSES = 56
TABLE_ROWS = 64


def f32(*shape):
    return jax.ShapeDtypeStruct(shape, jnp.float32)


def i32(*shape):
    return jax.ShapeDtypeStruct(shape, jnp.int32)


def call(kernel, outs, *args, in_specs=None, out_specs=None, scratch=()):
    return pl.pallas_call(
        kernel,
        out_shape=outs,
        in_specs=in_specs or [VMEM] * len(args),
        out_specs=out_specs or [VMEM] * len(outs),
        scratch_shapes=list(scratch),
        compiler_params=pltpu.CompilerParams(vmem_limit_bytes=GRANT),
    )(*args)


def take(block, lanes):
    return jnp.take_along_axis(block, lanes, axis=1, mode="promise_in_bounds")


class Chosen:
    def __init__(self, flag, if_set, if_clear):
        self.flag, self.if_set, self.if_clear = flag, if_set, if_clear

    def __getitem__(self, at):
        return jnp.where(self.flag, self.if_set[at], self.if_clear[at])


def write_pair(table, flag_row, up, down, inner, outer, rows):
    upper = table[flag_row : flag_row + 8, :] > 0
    for row in range(0, rows, 8):
        high = up[row : row + 8, :]
        low = down[row : row + 8, :]
        inner[row : row + 8, :] = jnp.where(upper, low, high)
        outer[row : row + 8, :] = jnp.where(upper, high, low)


def write_faces(values, up, down):
    up[0:64, :] = values[448:512, :]
    down[0:64, :] = values[0:64, :]
    for x in range(8):
        up[64 + 8 * x : 72 + 8 * x, :] = values[64 * x + 56 : 64 * x + 64, :]
        down[64 + 8 * x : 72 + 8 * x, :] = values[64 * x : 64 * x + 8, :]
    up[128:192, :] = values[pl.ds(7, 64, stride=8), :]
    down[128:192, :] = values[pl.ds(0, 64, stride=8), :]


def write_coarse_faces(values, at, faces, to):
    faces[to : to + 16, :] = values[at : at + 16, :]
    faces[to + 16 : to + 32, :] = values[at + 48 : at + 64, :]
    for x in range(4):
        faces[to + 32 + 4 * x : to + 36 + 4 * x, :] = values[at + 16 * x : at + 16 * x + 4, :]
        faces[to + 48 + 4 * x : to + 52 + 4 * x, :] = values[at + 16 * x + 12 : at + 16 * x + 16, :]
    faces[to + 64 : to + 80, :] = values[pl.ds(at, 16, stride=4), :]
    faces[to + 80 : to + 96, :] = values[pl.ds(at + 3, 16, stride=4), :]


def read_coarse_ghosts(faces, block, slots, device, ghosts):
    for face in range(6):
        slot = jnp.broadcast_to(slots[face : face + 1, :], (8, LANES))
        safe = jnp.maximum(slot, 0)
        lane = safe & (LANES - 1)
        distance = jnp.where(slot >= 0, jnp.abs(lax.shift_right_logical(safe, 7) - device), -1)
        for step in (0, 8):
            picked = jnp.zeros((8, LANES), jnp.float32)
            for which in range(REACH + 1):
                source = block - which if face % 2 == 0 else block + which
                row = 96 * source + 16 * (face ^ 1) + step
                picked = jnp.where(distance == which, take(faces[row : row + 8, :], lane), picked)
            ghosts[16 * face + step : 16 * face + step + 8, :] = picked


def windows_of(table, up, down, near_inner, near_outer, far_inner, far_outer):
    near = table[UPPER_NEAR : UPPER_NEAR + 8, :] > 0
    far = table[UPPER_FAR : UPPER_FAR + 8, :] > 0
    return (
        (up, Chosen(near, near_inner, near_outer), Chosen(far, far_inner, far_outer)),
        (down, Chosen(near, near_outer, near_inner), Chosen(far, far_outer, far_inner)),
    )


def read_ghosts(table, faces, ghosts, rows):
    windows = windows_of(table, *faces)
    per_face = rows // 3
    packed = rows // 2
    for face in range(6):
        own, near, far = windows[face % 2]
        lane = jnp.broadcast_to(table[LANE_ROW + face : LANE_ROW + face + 1, :], (8, LANES))
        window = jnp.broadcast_to(table[WINDOW_ROW + face : WINDOW_ROW + face + 1, :], (8, LANES))
        is_own, is_near, is_far, is_last = [window == which for which in range(4)]
        first_half = jnp.minimum(lane, TAIL - 1)
        second_half = first_half + TAIL
        for step in range(0, per_face, 8):
            row = (face // 2) * per_face + step
            last_row = rows + row % packed
            last_lane = first_half if row < packed else second_half
            picked = jnp.where(is_last, take(far[last_row : last_row + 8, :], last_lane), 0.0)
            picked = jnp.where(is_far, take(far[row : row + 8, :], lane), picked)
            picked = jnp.where(is_near, take(near[row : row + 8, :], lane), picked)
            picked = jnp.where(is_own, take(own[row : row + 8, :], lane), picked)
            ghosts[face * per_face + step : face * per_face + step + 8, :] = picked


def beside(values, ghosts, x, y):
    sub = lax.broadcasted_iota(jnp.int32, (8, LANES), 0)
    at = 64 * x + 8 * y
    line = 8 * x + y
    centre = values[at : at + 8, :]
    below_x = values[at - 64 : at - 56, :] if x > 0 else ghosts[8 * y : 8 * y + 8, :]
    above_x = values[at + 64 : at + 72, :] if x < 7 else ghosts[64 + 8 * y : 72 + 8 * y, :]
    below_y = values[at - 8 : at, :] if y > 0 else ghosts[128 + 8 * x : 136 + 8 * x, :]
    above_y = values[at + 8 : at + 16, :] if y < 7 else ghosts[192 + 8 * x : 200 + 8 * x, :]
    below_z = jnp.where(sub == 0, ghosts[256 + line : 257 + line, :], pltpu.roll(centre, 1, 0))
    above_z = jnp.where(sub == 7, ghosts[320 + line : 321 + line, :], pltpu.roll(centre, 7, 0))
    return centre, ((above_x + below_x) + (above_y + below_y)) + (above_z + below_z)


def start_kernel(row_length, device_ref, counts_ref, right_ref, neighbours_ref, residual, up, down, inner, outer, table):
    device = device_ref[0]
    own_count = counts_ref[device]
    lane = lax.broadcasted_iota(jnp.int32, (8, LANES), 1)
    live = lane < own_count
    for row in range(0, 512, 8):
        residual[row : row + 8, :] = jnp.where(live, right_ref[row : row + 8, :], 0.0)
    write_faces(residual, up, down)
    table[UPPER_NEAR : UPPER_NEAR + 8, :] = jnp.full((8, LANES), device & 1, jnp.int32)
    table[UPPER_FAR : UPPER_FAR + 8, :] = jnp.full((8, LANES), device & 2, jnp.int32)
    place = lax.rem(device, row_length)
    crosses = jnp.where((place == 0) | (place == row_length - 1), 1, 0)
    table[CROSSES : CROSSES + 8, :] = jnp.full((8, LANES), crosses, jnp.int32)
    write_pair(table, UPPER_NEAR, up, down, inner, outer, FINE)
    slot = neighbours_ref[...]
    present = slot >= 0
    slot = jnp.where(present, slot, 0)
    distance = jnp.abs(lax.shift_right_logical(slot, 7) - device)
    offset = slot & (LANES - 1)
    face = lax.broadcasted_iota(jnp.int32, (6, LANES), 0)
    skipped = jnp.maximum(counts_ref[jnp.maximum(device - 3, 0)] - TAIL, 0)
    shifted = jnp.where((distance == 3) & (face % 2 == 0), offset - skipped, offset)
    table[LANE_ROW : LANE_ROW + 6, :] = jnp.clip(shifted, 0, LANES - 1)
    table[WINDOW_ROW : WINDOW_ROW + 6, :] = jnp.where(present, distance, -1)
    table[NEIGHBOUR_ROW : NEIGHBOUR_ROW + 6, :] = neighbours_ref[...]
    table[NEIGHBOUR_ROW + 6 : NEIGHBOUR_ROW + 8, :] = jnp.full((2, LANES), -1, jnp.int32)
    forward = jnp.maximum(counts_ref[jnp.maximum(device - 1, 0)] - TAIL, 0)
    table[FORWARD_UP : FORWARD_UP + 8, :] = (lane & (TAIL - 1)) + forward
    table[FORWARD_DOWN : FORWARD_DOWN + 8, :] = lane & (TAIL - 1)


def pack(rows, flag_row, table, up, down, near_up, near_down, message):
    half = rows // 2
    lane = lax.broadcasted_iota(jnp.int32, (8, LANES), 1)
    upper = table[UPPER_FAR : UPPER_FAR + 8, :] > 0
    downwards = upper if flag_row else jnp.logical_not(upper)
    lanes_up = table[FORWARD_UP : FORWARD_UP + 8, :]
    lanes_down = table[FORWARD_DOWN : FORWARD_DOWN + 8, :]
    lanes = jnp.where(downwards, lanes_down, lanes_up)
    own = Chosen(downwards, down, up)
    near = Chosen(downwards, near_down, near_up)
    for row in range(0, rows, 8):
        message[row : row + 8, :] = own[row : row + 8, :]
    for row in range(0, half, 8):
        first = take(near[row : row + 8, :], lanes)
        second = take(near[half + row : half + row + 8, :], lanes)
        message[rows + row : rows + row + 8, :] = jnp.where(lane < TAIL, first, second)


def pack_outer_kernel(rows, up, down, near_inner, near_outer, table, message):
    near = table[UPPER_NEAR : UPPER_NEAR + 8, :] > 0
    near_up = Chosen(near, near_inner, near_outer)
    near_down = Chosen(near, near_outer, near_inner)
    pack(rows, False, table, up, down, near_up, near_down, message)


def pack_inner_kernel(rows, up, down, near_inner, near_outer, near_across, table, message, merged):
    near = table[UPPER_NEAR : UPPER_NEAR + 8, :] > 0
    either = Chosen(table[CROSSES : CROSSES + 8, :] > 0, near_across, near_outer)
    for row in range(0, rows, 8):
        merged[row : row + 8, :] = either[row : row + 8, :]
    near_up = Chosen(near, near_inner, merged)
    near_down = Chosen(near, merged, near_inner)
    pack(rows, True, table, up, down, near_up, near_down, message)


def smooth_kernel(residual, *refs):
    *faces, table, out, out_up, out_down, out_inner, out_outer, ghosts = refs
    read_ghosts(table, faces, ghosts, FINE)
    for x in range(8):
        for y in range(8):
            centre, around = beside(residual, ghosts, x, y)
            first = RELAX_FINE * centre
            applied = 6.0 * first - RELAX_FINE * around
            at = 64 * x + 8 * y
            out[at : at + 8, :] = first + RELAX_FINE * (centre - applied)
    write_faces(out, out_up, out_down)
    write_pair(table, UPPER_NEAR, out_up, out_down, out_inner, out_outer, FINE)


def defect_kernel(residual, second, *refs):
    *faces, table, defect, block, ghosts, sums = refs
    read_ghosts(table, faces, ghosts, FINE)
    for big_x in range(4):
        for big_y in range(4):
            total = None
            for x in (2 * big_x, 2 * big_x + 1):
                for y in (2 * big_y, 2 * big_y + 1):
                    centre, around = beside(second, ghosts, x, y)
                    at = 64 * x + 8 * y
                    part = residual[at : at + 8, :] - (6.0 * centre - around)
                    defect[at : at + 8, :] = part
                    total = part if total is None else total + part
            at = 32 * big_x + 8 * big_y
            sums[at : at + 8, :] = total
    restricted = (sums[pl.ds(0, 64, stride=2), :] + sums[pl.ds(1, 64, stride=2), :]) * 0.125
    block[0:64, :] = restricted
    block[64:72, :] = table[NEIGHBOUR_ROW : NEIGHBOUR_ROW + 8, :].astype(jnp.float32)


def spread_kernel(device_ref, own, across, beside_row, out):
    column = device_ref[0] % out.shape[0]
    odd_row = (device_ref[0] // out.shape[0]) % 2
    for target in range(out.shape[0]):
        out[target, 0:BLOCK, :] = own[...]
        from_before = jnp.where(column > target, 1, 0)
        same = jnp.full((8, LANES), jnp.where(odd_row == from_before, 1, 0), jnp.int32) > 0
        for row in range(0, BLOCK, 8):
            other = jnp.where(same, beside_row[row : row + 8, :], across[row : row + 8, :])
            out[target, BLOCK + row : BLOCK + row + 8, :] = other


def coarse_update(first, at, ghosts, low_y, high_y, low_z, high_z):
    for x in range(4):
        low_y[16 * x : 16 * x + 4, :] = ghosts[32 + 4 * x : 36 + 4 * x, :]
        high_y[16 * x + 12 : 16 * x + 16, :] = ghosts[48 + 4 * x : 52 + 4 * x, :]
    low_z[pl.ds(0, 16, stride=4), :] = ghosts[64:80, :]
    high_z[pl.ds(3, 16, stride=4), :] = ghosts[80:96, :]
    centre = first[at : at + 64, :]
    row = lax.broadcasted_iota(jnp.int32, (64, LANES), 0)
    below_x = jnp.concatenate([ghosts[0:16, :], first[at : at + 48, :]], axis=0)
    above_x = jnp.concatenate([first[at + 16 : at + 64, :], ghosts[16:32, :]], axis=0)
    below_y = jnp.where((row & 15) < 4, low_y[...], pltpu.roll(centre, 4, 0))
    above_y = jnp.where((row & 15) >= 12, high_y[...], pltpu.roll(centre, 60, 0))
    below_z = jnp.where((row & 3) == 0, low_z[...], pltpu.roll(centre, 1, 0))
    above_z = jnp.where((row & 3) == 3, high_z[...], pltpu.roll(centre, 63, 0))
    around = ((above_x + below_x) + (above_y + below_y)) + (above_z + below_z)
    return centre + (centre - RELAX_COARSE * ((6.0 * centre - around) * 0.25))


def correct_kernel(device_ref, second, defect, received, *refs):
    table, out, out_up, out_down, out_inner, out_outer, *scratch = refs
    first, first_faces, slots, coarse, coarse_faces, ghosts, low_y, high_y, low_z, high_z, *scratch = scratch
    wide, wide_ghosts, spread = scratch
    device = device_ref[0]
    row_length = received.shape[0]
    column = device % row_length
    for block in range(4 * REACH + 1):
        place = column + (block - 2 * REACH)
        in_row = (place >= 0) & (place < row_length)
        sender = lax.rem(place + row_length, row_length)
        start = jnp.where(in_row, 0, BLOCK)
        for row in range(0, 64, 8):
            at = pl.multiple_of(start + row, 8)
            first[64 * block + row : 64 * block + row + 8, :] = RELAX_COARSE * received[sender, pl.ds(at, 8), :]
        write_coarse_faces(first, 64 * block, first_faces, 96 * block)
        if REACH <= block <= 3 * REACH:
            at = pl.multiple_of(start + 64, 8)
            to = 8 * (block - REACH)
            slots[to : to + 8, :] = received[sender, pl.ds(at, 8), :].astype(jnp.int32)
    for block in range(2 * REACH + 1):
        block_slots = slots.at[8 * block : 8 * block + 8, :]
        read_coarse_ghosts(first_faces, block + REACH, block_slots, device + (block - REACH), ghosts)
        updated = coarse_update(first, 64 * (block + REACH), ghosts, low_y, high_y, low_z, high_z)
        coarse[64 * block : 64 * block + 64, :] = updated
        write_coarse_faces(coarse, 64 * block, coarse_faces, 96 * block)
    read_coarse_ghosts(coarse_faces, REACH, slots.at[8 * REACH : 8 * REACH + 8, :], device, ghosts)
    own = coarse[64 * REACH : 64 * REACH + 64, :]
    wide[pl.ds(0, 64, stride=2), :] = own
    wide[pl.ds(1, 64, stride=2), :] = own
    wide_ghosts[pl.ds(0, 64, stride=2), :] = ghosts[0:64, :]
    wide_ghosts[pl.ds(1, 64, stride=2), :] = ghosts[0:64, :]
    for x in range(8):
        for y in range(8):
            at = 64 * x + 8 * y
            source = 32 * (x // 2) + 8 * (y // 2)
            spread[at : at + 8, :] = wide[source : source + 8, :]
    sub = lax.broadcasted_iota(jnp.int32, (8, LANES), 0)
    for x in range(8):
        for y in range(8):
            at = 64 * x + 8 * y
            cell = 4 * (x // 2) + y // 2
            centre = spread[at : at + 8, :]
            side_x = 8 * (y // 2)
            side_y = 8 * (x // 2)
            below_x = spread[at - 64 : at - 56, :] if x > 0 else wide_ghosts[side_x : side_x + 8, :]
            above_x = spread[at + 64 : at + 72, :] if x < 7 else wide_ghosts[32 + side_x : 40 + side_x, :]
            below_y = spread[at - 8 : at, :] if y > 0 else wide_ghosts[64 + side_y : 72 + side_y, :]
            above_y = spread[at + 8 : at + 16, :] if y < 7 else wide_ghosts[96 + side_y : 104 + side_y, :]
            below_z = jnp.where(sub == 0, ghosts[64 + cell : 65 + cell, :], pltpu.roll(centre, 1, 0))
            above_z = jnp.where(sub == 7, ghosts[80 + cell : 81 + cell, :], pltpu.roll(centre, 7, 0))
            around = ((above_x + below_x) + (above_y + below_y)) + (above_z + below_z)
            left = defect[at : at + 8, :] - (6.0 * centre - around)
            out[at : at + 8, :] = (second[at : at + 8, :] + centre) + RELAX_FINE * left
    write_faces(out, out_up, out_down)
    write_pair(table, UPPER_NEAR, out_up, out_down, out_inner, out_outer, FINE)


def image_kernel(residual, direction, *refs):
    *faces, table, image, sums, ghosts = refs
    read_ghosts(table, faces, ghosts, FINE)
    zero = jnp.zeros((8, LANES), jnp.float32)
    parts = [zero] * 5
    for x in range(8):
        for y in range(8):
            centre, around = beside(direction, ghosts, x, y)
            at = 64 * x + 8 * y
            applied = 6.0 * centre - around
            image[at : at + 8, :] = applied
            start = residual[at : at + 8, :]
            terms = (start * centre, centre * applied, start * start, start * applied, applied * applied)
            parts = [part + term for part, term in zip(parts, terms)]
    lane = lax.broadcasted_iota(jnp.int32, (1, LANES), 1)
    row = jnp.zeros((1, LANES), jnp.float32)
    for index, part in enumerate(parts):
        row = jnp.where(lane == index, jnp.sum(part), row)
    for copy in range(sums.shape[0]):
        sums[copy] = row


def add_kernel(received, out):
    total = received[0]
    for index in range(1, received.shape[0]):
        total = total + received[index]
    for copy in range(out.shape[0]):
        out[copy] = total


def finish_kernel(received, residual, direction, image, solution, left, norm):
    total = received[0]
    for index in range(1, received.shape[0]):
        total = total + received[index]
    lane = lax.broadcasted_iota(jnp.int32, (1, LANES), 1)
    along, curvature, old_square, cross_term, image_square = [
        jnp.full((8, LANES), jnp.sum(jnp.where(lane == index, total, 0.0)), jnp.float32) for index in range(5)
    ]
    step_size = along / curvature
    for row in range(0, 512, 8):
        solution[row : row + 8, :] = step_size * direction[row : row + 8, :]
        left[row : row + 8, :] = residual[row : row + 8, :] - step_size * image[row : row + 8, :]
    norm[...] = jnp.sqrt(old_square - 2.0 * step_size * cross_term + step_size * step_size * image_square)


def swap(block, distance, offset, keep=lambda low: True):
    count = lax.axis_size(AXES)
    route = []
    for low in range(count - distance):
        if (low - offset) % (2 * distance) < distance and keep(low):
            route += [(low, low + distance), (low + distance, low)]
    return lax.ppermute(block, AXES, route)


def exchange(rows, up, down, inner, outer, table):
    row_length = lax.axis_size("row")
    crosses = lambda low: low % row_length == row_length - 1
    message = f32(rows + rows // 2, LANES)
    near_outer = swap(outer, 1, 1, lambda low: not crosses(low))
    near_inner = swap(inner, 1, 0)
    near_across = swap(outer, 1, 1, crosses)
    (outer,) = call(functools.partial(pack_outer_kernel, rows), [message], up, down, near_inner, near_outer, table)
    far_outer = swap(outer, 2, 2)
    inner, near_outer = call(
        functools.partial(pack_inner_kernel, rows), [message, f32(rows, LANES)],
        up, down, near_inner, near_outer, near_across, table,
    )
    far_inner = swap(inner, 2, 0)
    return up, down, near_inner, near_outer, far_inner, far_outer, table


def share(block, device):
    row_length = lax.axis_size("row")
    across = swap(block, row_length, row_length)
    beside_row = swap(block, row_length, 0)
    (blocks,) = call(
        spread_kernel, [f32(row_length, 2 * BLOCK, LANES)], device, block, across, beside_row,
        in_specs=[SMEM, VMEM, VMEM, VMEM],
    )
    return lax.all_to_all(blocks, "row", 0, 0, tiled=True)


def step(right_side, counts, neighbours):
    device = lax.axis_index(AXES).astype(jnp.int32).reshape(1)
    fine = f32(512, LANES)
    faces = [f32(FINE, LANES)] * 4
    fine_ghosts = pltpu.VMEM((2 * FINE, LANES), jnp.float32)
    scratch = lambda rows: pltpu.VMEM((rows, LANES), jnp.float32)

    residual_in, *sides, table = call(
        functools.partial(start_kernel, lax.axis_size("row")), [fine, *faces, i32(TABLE_ROWS, LANES)], device, counts, right_side, neighbours,
        in_specs=[SMEM, SMEM, VMEM, VMEM],
    )
    second, *sides = call(
        smooth_kernel, [fine, *faces], residual_in, *exchange(FINE, *sides, table), scratch=[fine_ghosts]
    )
    defect, block = call(
        defect_kernel, [fine, f32(BLOCK, LANES)],
        residual_in, second, *exchange(FINE, *sides, table), scratch=[fine_ghosts, scratch(128)],
    )
    blocks = 2 * REACH + 1
    direction, *sides = call(
        correct_kernel, [fine, *faces], device, second, defect, share(block, device), table,
        in_specs=[SMEM] + [VMEM] * 4,
        scratch=[
            scratch(64 * (4 * REACH + 1)), scratch(96 * (4 * REACH + 1)), pltpu.VMEM((8 * blocks, LANES), jnp.int32),
            scratch(64 * blocks), scratch(96 * blocks), scratch(96), *[scratch(64)] * 4,
            scratch(128), scratch(128), scratch(512),
        ],
    )
    image, sums = call(
        image_kernel, [fine, f32(lax.axis_size(AXES[1:]), 1, LANES)],
        residual_in, direction, *exchange(FINE, *sides, table), scratch=[fine_ghosts],
    )
    received = lax.all_to_all(sums, AXES[1:], 0, 0, tiled=True)
    (sums,) = call(add_kernel, [f32(lax.axis_size("outer"), 1, LANES)], received)
    received = lax.all_to_all(sums, "outer", 0, 0, tiled=True)
    solved, left, norm = call(finish_kernel, [fine, fine, f32(8, LANES)], received, residual_in, direction, image)
    return solved, left, norm[0, 0]


def solution(mesh):
    devices = mesh.devices.reshape(-1, PAIR, mesh.shape["level"])
    split = Mesh(devices, AXES)
    return jax.shard_map(
        step,
        mesh=split,
        in_specs=(P(None, AXES), P(), P(None, AXES)),
        out_specs=(P(None, AXES), P(None, AXES), P()),
        check_vma=False,
    )
```

```python
import functools

import jax
import jax.numpy as jnp
from jax import lax
from jax.experimental import pallas as pl
from jax.experimental.pallas import tpu as pltpu
from jax.sharding import Mesh
from jax.sharding import PartitionSpec as P


LANES = 128
TAIL = 64
FINE = 192
PAIR = 2
BLOCK = 72
REACH = 3
WIDEST = 8
GRANT = 8 * 1024 * 1024
AXES = ("outer", "pair", "row")
RELAX_FINE = (2.0 / 3.0) / 6.0
RELAX_COARSE = (2.0 / 3.0) / 1.5

VMEM = pl.BlockSpec(memory_space=pltpu.VMEM)
SMEM = pl.BlockSpec(memory_space=pltpu.SMEM)

LANE_ROW = 0
WINDOW_ROW = 8
FORWARD_UP = 16
FORWARD_DOWN = 24
UPPER_NEAR = 32
UPPER_FAR = 40
NEIGHBOUR_ROW = 48
CROSSES = 56
TABLE_ROWS = 64


def f32(*shape):
    return jax.ShapeDtypeStruct(shape, jnp.float32)


def i32(*shape):
    return jax.ShapeDtypeStruct(shape, jnp.int32)


def call(kernel, outs, *args, in_specs=None, out_specs=None, scratch=()):
    return pl.pallas_call(
        kernel,
        out_shape=outs,
        in_specs=in_specs or [VMEM] * len(args),
        out_specs=out_specs or [VMEM] * len(outs),
        scratch_shapes=list(scratch),
        compiler_params=pltpu.CompilerParams(vmem_limit_bytes=GRANT),
    )(*args)


def take(block, lanes):
    return jnp.take_along_axis(block, lanes, axis=1, mode="promise_in_bounds")


class Chosen:
    def __init__(self, flag, if_set, if_clear):
        self.flag, self.if_set, self.if_clear = flag, if_set, if_clear

    def __getitem__(self, at):
        return jnp.where(self.flag, self.if_set[at], self.if_clear[at])


def write_pair(table, flag_row, up, down, inner, outer, rows):
    upper = table[flag_row : flag_row + 8, :] > 0
    for row in range(0, rows, 8):
        high = up[row : row + 8, :]
        low = down[row : row + 8, :]
        inner[row : row + 8, :] = jnp.where(upper, low, high)
        outer[row : row + 8, :] = jnp.where(upper, high, low)


def write_faces(values, up, down):
    up[0:64, :] = values[448:512, :]
    down[0:64, :] = values[0:64, :]
    for x in range(8):
        up[64 + 8 * x : 72 + 8 * x, :] = values[64 * x + 56 : 64 * x + 64, :]
        down[64 + 8 * x : 72 + 8 * x, :] = values[64 * x : 64 * x + 8, :]
    up[128:192, :] = values[pl.ds(7, 64, stride=8), :]
    down[128:192, :] = values[pl.ds(0, 64, stride=8), :]


def write_coarse_faces(values, at, faces, to):
    faces[to : to + 16, :] = values[at : at + 16, :]
    faces[to + 16 : to + 32, :] = values[at + 48 : at + 64, :]
    for x in range(4):
        faces[to + 32 + 4 * x : to + 36 + 4 * x, :] = values[at + 16 * x : at + 16 * x + 4, :]
        faces[to + 48 + 4 * x : to + 52 + 4 * x, :] = values[at + 16 * x + 12 : at + 16 * x + 16, :]
    faces[to + 64 : to + 80, :] = values[pl.ds(at, 16, stride=4), :]
    faces[to + 80 : to + 96, :] = values[pl.ds(at + 3, 16, stride=4), :]


def read_planes(planes, rows, block, slots, device, out):
    blocks = planes.shape[0] // (6 * rows)
    for face in range(6):
        slot = jnp.broadcast_to(slots[face : face + 1, :], (8, LANES))
        safe = jnp.maximum(slot, 0)
        lane = safe & (LANES - 1)
        distance = jnp.where(slot >= 0, jnp.abs(lax.shift_right_logical(safe, 7) - device), -1)
        for step in range(0, rows, 8):
            picked = jnp.zeros((8, LANES), jnp.float32)
            for which in range(REACH + 1):
                source = block - which if face % 2 == 0 else block + which
                if 0 <= source < blocks:
                    row = rows * (6 * source + (face ^ 1)) + step
                    picked = jnp.where(distance == which, take(planes[row : row + 8, :], lane), picked)
            out[rows * face + step : rows * face + step + 8, :] = picked


def write_rims(faces, at, ghosts, extended, to):
    for face in range(6):
        axis, side = face // 2, 3 * (face % 2)
        row = to + 32 * face
        extended[row : row + 16, :] = faces[at + 16 * face : at + 16 * face + 16, :]
        row += 16
        for other in (other for other in range(3) if other != axis):
            along = 3 - axis - other
            for lateral in (2 * other, 2 * other + 1):
                if axis < along:
                    edge = ghosts[16 * lateral + 4 * side : 16 * lateral + 4 * side + 4, :]
                else:
                    edge = ghosts[pl.ds(16 * lateral + side, 4, stride=4), :]
                extended[row : row + 4, :] = edge
                row += 4


def windows_of(table, up, down, near_inner, near_outer, far_inner, far_outer):
    near = table[UPPER_NEAR : UPPER_NEAR + 8, :] > 0
    far = table[UPPER_FAR : UPPER_FAR + 8, :] > 0
    return (
        (up, Chosen(near, near_inner, near_outer), Chosen(far, far_inner, far_outer)),
        (down, Chosen(near, near_outer, near_inner), Chosen(far, far_outer, far_inner)),
    )


def read_ghosts(table, faces, ghosts, rows):
    windows = windows_of(table, *faces)
    per_face = rows // 3
    packed = rows // 2
    for face in range(6):
        own, near, far = windows[face % 2]
        lane = jnp.broadcast_to(table[LANE_ROW + face : LANE_ROW + face + 1, :], (8, LANES))
        window = jnp.broadcast_to(table[WINDOW_ROW + face : WINDOW_ROW + face + 1, :], (8, LANES))
        is_own, is_near, is_far, is_last = [window == which for which in range(4)]
        first_half = jnp.minimum(lane, TAIL - 1)
        second_half = first_half + TAIL
        for step in range(0, per_face, 8):
            row = (face // 2) * per_face + step
            last_row = rows + row % packed
            last_lane = first_half if row < packed else second_half
            picked = jnp.where(is_last, take(far[last_row : last_row + 8, :], last_lane), 0.0)
            picked = jnp.where(is_far, take(far[row : row + 8, :], lane), picked)
            picked = jnp.where(is_near, take(near[row : row + 8, :], lane), picked)
            picked = jnp.where(is_own, take(own[row : row + 8, :], lane), picked)
            ghosts[face * per_face + step : face * per_face + step + 8, :] = picked


def beside(values, ghosts, x, y):
    sub = lax.broadcasted_iota(jnp.int32, (8, LANES), 0)
    at = 64 * x + 8 * y
    line = 8 * x + y
    centre = values[at : at + 8, :]
    below_x = values[at - 64 : at - 56, :] if x > 0 else ghosts[8 * y : 8 * y + 8, :]
    above_x = values[at + 64 : at + 72, :] if x < 7 else ghosts[64 + 8 * y : 72 + 8 * y, :]
    below_y = values[at - 8 : at, :] if y > 0 else ghosts[128 + 8 * x : 136 + 8 * x, :]
    above_y = values[at + 8 : at + 16, :] if y < 7 else ghosts[192 + 8 * x : 200 + 8 * x, :]
    below_z = jnp.where(sub == 0, ghosts[256 + line : 257 + line, :], pltpu.roll(centre, 1, 0))
    above_z = jnp.where(sub == 7, ghosts[320 + line : 321 + line, :], pltpu.roll(centre, 7, 0))
    return centre, ((above_x + below_x) + (above_y + below_y)) + (above_z + below_z)


def start_kernel(row_length, device_ref, counts_ref, right_ref, neighbours_ref, residual, up, down, inner, outer, table):
    device = device_ref[0]
    own_count = counts_ref[device]
    lane = lax.broadcasted_iota(jnp.int32, (8, LANES), 1)
    live = lane < own_count
    for row in range(0, 512, 8):
        residual[row : row + 8, :] = jnp.where(live, right_ref[row : row + 8, :], 0.0)
    write_faces(residual, up, down)
    table[UPPER_NEAR : UPPER_NEAR + 8, :] = jnp.full((8, LANES), device & 1, jnp.int32)
    table[UPPER_FAR : UPPER_FAR + 8, :] = jnp.full((8, LANES), device & 2, jnp.int32)
    place = lax.rem(device, row_length)
    crosses = jnp.where((place == 0) | (place == row_length - 1), 1, 0)
    table[CROSSES : CROSSES + 8, :] = jnp.full((8, LANES), crosses, jnp.int32)
    write_pair(table, UPPER_NEAR, up, down, inner, outer, FINE)
    slot = neighbours_ref[...]
    present = slot >= 0
    slot = jnp.where(present, slot, 0)
    distance = jnp.abs(lax.shift_right_logical(slot, 7) - device)
    offset = slot & (LANES - 1)
    face = lax.broadcasted_iota(jnp.int32, (6, LANES), 0)
    skipped = jnp.maximum(counts_ref[jnp.maximum(device - 3, 0)] - TAIL, 0)
    shifted = jnp.where((distance == 3) & (face % 2 == 0), offset - skipped, offset)
    table[LANE_ROW : LANE_ROW + 6, :] = jnp.clip(shifted, 0, LANES - 1)
    table[WINDOW_ROW : WINDOW_ROW + 6, :] = jnp.where(present, distance, -1)
    table[NEIGHBOUR_ROW : NEIGHBOUR_ROW + 6, :] = neighbours_ref[...]
    table[NEIGHBOUR_ROW + 6 : NEIGHBOUR_ROW + 8, :] = jnp.full((2, LANES), -1, jnp.int32)
    forward = jnp.maximum(counts_ref[jnp.maximum(device - 1, 0)] - TAIL, 0)
    table[FORWARD_UP : FORWARD_UP + 8, :] = (lane & (TAIL - 1)) + forward
    table[FORWARD_DOWN : FORWARD_DOWN + 8, :] = lane & (TAIL - 1)


def pack(rows, flag_row, table, up, down, near_up, near_down, message):
    half = rows // 2
    lane = lax.broadcasted_iota(jnp.int32, (8, LANES), 1)
    upper = table[UPPER_FAR : UPPER_FAR + 8, :] > 0
    downwards = upper if flag_row else jnp.logical_not(upper)
    lanes_up = table[FORWARD_UP : FORWARD_UP + 8, :]
    lanes_down = table[FORWARD_DOWN : FORWARD_DOWN + 8, :]
    lanes = jnp.where(downwards, lanes_down, lanes_up)
    own = Chosen(downwards, down, up)
    near = Chosen(downwards, near_down, near_up)
    for row in range(0, rows, 8):
        message[row : row + 8, :] = own[row : row + 8, :]
    for row in range(0, half, 8):
        first = take(near[row : row + 8, :], lanes)
        second = take(near[half + row : half + row + 8, :], lanes)
        message[rows + row : rows + row + 8, :] = jnp.where(lane < TAIL, first, second)


def pack_outer_kernel(rows, up, down, near_inner, near_outer, table, message):
    near = table[UPPER_NEAR : UPPER_NEAR + 8, :] > 0
    near_up = Chosen(near, near_inner, near_outer)
    near_down = Chosen(near, near_outer, near_inner)
    pack(rows, False, table, up, down, near_up, near_down, message)


def pack_inner_kernel(rows, up, down, near_inner, near_outer, near_across, table, message, merged):
    near = table[UPPER_NEAR : UPPER_NEAR + 8, :] > 0
    either = Chosen(table[CROSSES : CROSSES + 8, :] > 0, near_across, near_outer)
    for row in range(0, rows, 8):
        merged[row : row + 8, :] = either[row : row + 8, :]
    near_up = Chosen(near, near_inner, merged)
    near_down = Chosen(near, merged, near_inner)
    pack(rows, True, table, up, down, near_up, near_down, message)


def smooth_kernel(residual, *refs):
    *faces, table, out, out_up, out_down, out_inner, out_outer, ghosts = refs
    read_ghosts(table, faces, ghosts, FINE)
    for x in range(8):
        for y in range(8):
            centre, around = beside(residual, ghosts, x, y)
            first = RELAX_FINE * centre
            applied = 6.0 * first - RELAX_FINE * around
            at = 64 * x + 8 * y
            out[at : at + 8, :] = first + RELAX_FINE * (centre - applied)
    write_faces(out, out_up, out_down)
    write_pair(table, UPPER_NEAR, out_up, out_down, out_inner, out_outer, FINE)


def defect_kernel(residual, second, *refs):
    *faces, table, smoothed, block, out_up, out_down, out_inner, out_outer, ghosts, sums = refs
    read_ghosts(table, faces, ghosts, FINE)
    for big_x in range(4):
        for big_y in range(4):
            total = None
            for x in (2 * big_x, 2 * big_x + 1):
                for y in (2 * big_y, 2 * big_y + 1):
                    centre, around = beside(second, ghosts, x, y)
                    at = 64 * x + 8 * y
                    part = residual[at : at + 8, :] - (6.0 * centre - around)
                    smoothed[at : at + 8, :] = centre + RELAX_FINE * part
                    total = part if total is None else total + part
            at = 32 * big_x + 8 * big_y
            sums[at : at + 8, :] = total
    block[0:64, :] = (sums[pl.ds(0, 64, stride=2), :] + sums[pl.ds(1, 64, stride=2), :]) * 0.125
    block[64:72, :] = table[NEIGHBOUR_ROW : NEIGHBOUR_ROW + 8, :].astype(jnp.float32)
    write_faces(smoothed, out_up, out_down)
    write_pair(table, UPPER_NEAR, out_up, out_down, out_inner, out_outer, FINE)


def spread_kernel(device_ref, own, across, beside_row, out):
    column = device_ref[0] % out.shape[0]
    odd_row = (device_ref[0] // out.shape[0]) % 2
    after_is_beside = jnp.full((8, LANES), odd_row, jnp.int32) == 0
    for target in range(out.shape[0]):
        stays = jnp.full((8, LANES), column, jnp.int32) == target
        from_before = jnp.where(column >= target, 1, 0)
        same = jnp.full((8, LANES), jnp.where(odd_row == from_before, 1, 0), jnp.int32) > 0
        for row in range(0, BLOCK, 8):
            near = beside_row[row : row + 8, :]
            far = across[row : row + 8, :]
            after = jnp.where(after_is_beside, near, far)
            out[target, row : row + 8, :] = jnp.where(stays, after, own[row : row + 8, :])
            out[target, BLOCK + row : BLOCK + row + 8, :] = jnp.where(same, near, far)


def coarse_update(first, at, ghosts, low_y, high_y, low_z, high_z):
    for x in range(4):
        low_y[16 * x : 16 * x + 4, :] = ghosts[32 + 4 * x : 36 + 4 * x, :]
        high_y[16 * x + 12 : 16 * x + 16, :] = ghosts[48 + 4 * x : 52 + 4 * x, :]
    low_z[pl.ds(0, 16, stride=4), :] = ghosts[64:80, :]
    high_z[pl.ds(3, 16, stride=4), :] = ghosts[80:96, :]
    centre = first[at : at + 64, :]
    row = lax.broadcasted_iota(jnp.int32, (64, LANES), 0)
    below_x = jnp.concatenate([ghosts[0:16, :], first[at : at + 48, :]], axis=0)
    above_x = jnp.concatenate([first[at + 16 : at + 64, :], ghosts[16:32, :]], axis=0)
    below_y = jnp.where((row & 15) < 4, low_y[...], pltpu.roll(centre, 4, 0))
    above_y = jnp.where((row & 15) >= 12, high_y[...], pltpu.roll(centre, 60, 0))
    below_z = jnp.where((row & 3) == 0, low_z[...], pltpu.roll(centre, 1, 0))
    above_z = jnp.where((row & 3) == 3, high_z[...], pltpu.roll(centre, 63, 0))
    around = ((above_x + below_x) + (above_y + below_y)) + (above_z + below_z)
    return centre + (centre - RELAX_COARSE * ((6.0 * centre - around) * 0.25))


def coarse_correction(device, block, received, scratch):
    first, first_faces, slots, coarse, coarse_faces, ghosts, low_y, high_y, low_z, high_z, extended, across = scratch
    row_length = received.shape[0]
    column = lax.rem(device, row_length)
    for index in range(2 * WIDEST + 1):
        offset = index - WIDEST
        if offset:
            place = column + offset
            sender = lax.rem(place + row_length, row_length)
            in_row = (place >= 0) & (place < row_length)
            start = 0 if offset == WIDEST else jnp.where(in_row, 0, BLOCK)
            rows = lambda row: received[sender, pl.ds(pl.multiple_of(start + row, 8), 8), :]
        else:
            rows = lambda row: block[row : row + 8, :]
        for row in range(0, 64, 8):
            first[64 * index + row : 64 * index + row + 8, :] = RELAX_COARSE * rows(row)
        write_coarse_faces(first, 64 * index, first_faces, 96 * index)
        if abs(offset) <= 2 * REACH:
            to = 8 * (offset + 2 * REACH)
            slots[to : to + 8, :] = rows(64).astype(jnp.int32)
    slots_of = lambda offset: slots.at[8 * (offset + 2 * REACH) : 8 * (offset + 2 * REACH) + 8, :]
    for offset in range(-2 * REACH, 2 * REACH + 1):
        index = offset + 2 * REACH
        read_planes(first_faces, 16, offset + WIDEST, slots_of(offset), device + offset, ghosts)
        updated = coarse_update(first, 64 * (offset + WIDEST), ghosts, low_y, high_y, low_z, high_z)
        coarse[...] = updated
        write_coarse_faces(coarse, 0, coarse_faces, 96 * index)
        if offset == 0:
            first[0:64, :] = updated
    for offset in range(-REACH, REACH + 1):
        index = offset + 2 * REACH
        read_planes(coarse_faces, 16, index, slots_of(offset), device + offset, ghosts)
        write_rims(coarse_faces, 96 * index, ghosts, extended, 192 * (offset + REACH))
    read_planes(extended, 32, REACH, slots_of(0), device, across)
    return first[0:64, :]


def image_kernel(device_ref, residual, smoothed, block, received, *refs):
    *faces, table, direction, image, sums, fine_ghosts, wide, wide_across, wide_own, spread = refs[: 7 + 3 + 5]
    scratch = refs[7 + 3 + 5 :]
    coarse_faces, across = scratch[4], scratch[-1]
    own = coarse_correction(device_ref[0], block, received, scratch)
    sub = lax.broadcasted_iota(jnp.int32, (8, LANES), 0)
    for half in (0, 1):
        wide[pl.ds(half, 64, stride=2), :] = own
        wide_across[pl.ds(half, 192, stride=2), :] = across[...]
        wide_own[pl.ds(half, 96, stride=2), :] = coarse_faces[192 * REACH : 192 * REACH + 96, :]
    for x in range(8):
        for y in range(8):
            at = 64 * x + 8 * y
            source = 32 * (x // 2) + 8 * (y // 2)
            spread[at : at + 8, :] = wide[source : source + 8, :]
    for x in range(8):
        for y in range(8):
            at = 64 * x + 8 * y
            cell = 4 * (x // 2) + y // 2
            centre = spread[at : at + 8, :]
            side_x = 8 * (y // 2)
            side_y = 8 * (x // 2)
            below_x = spread[at - 64 : at - 56, :] if x > 0 else wide_across[side_x : side_x + 8, :]
            above_x = spread[at + 64 : at + 72, :] if x < 7 else wide_across[64 + side_x : 72 + side_x, :]
            below_y = spread[at - 8 : at, :] if y > 0 else wide_across[128 + side_y : 136 + side_y, :]
            above_y = spread[at + 8 : at + 16, :] if y < 7 else wide_across[192 + side_y : 200 + side_y, :]
            below_z = jnp.where(sub == 0, across[128 + cell : 129 + cell, :], pltpu.roll(centre, 1, 0))
            above_z = jnp.where(sub == 7, across[160 + cell : 161 + cell, :], pltpu.roll(centre, 7, 0))
            around = ((above_x + below_x) + (above_y + below_y)) + (above_z + below_z)
            change = centre - RELAX_FINE * (6.0 * centre - around)
            direction[at : at + 8, :] = smoothed[at : at + 8, :] + change
    read_ghosts(table, faces, fine_ghosts, FINE)
    for face in range(6):
        for i in range(8):
            line = i // 2
            centre = wide_across[64 * face + 8 * line : 64 * face + 8 * line + 8, :]
            below = 64 * face + (8 * ((i - 1) // 2) if i > 0 else 32)
            above = 64 * face + (8 * ((i + 1) // 2) if i < 7 else 40)
            low = across[32 * face + 24 + line : 32 * face + 25 + line, :]
            high = across[32 * face + 28 + line : 32 * face + 29 + line, :]
            around = wide_across[below : below + 8, :] + wide_across[above : above + 8, :]
            around = around + jnp.where(sub == 0, low, pltpu.roll(centre, 1, 0))
            around = around + jnp.where(sub == 7, high, pltpu.roll(centre, 7, 0))
            around = around + wide_own[32 * face + 8 * line : 32 * face + 8 * line + 8, :]
            at = 64 * face + 8 * i
            change = centre - RELAX_FINE * (5.0 * centre - around)
            present = jnp.broadcast_to(table[WINDOW_ROW + face : WINDOW_ROW + face + 1, :], (8, LANES)) >= 0
            fine_ghosts[at : at + 8, :] = fine_ghosts[at : at + 8, :] + jnp.where(present, change, 0.0)
    zero = jnp.zeros((8, LANES), jnp.float32)
    parts = [zero] * 5
    for x in range(8):
        for y in range(8):
            centre, around = beside(direction, fine_ghosts, x, y)
            at = 64 * x + 8 * y
            applied = 6.0 * centre - around
            image[at : at + 8, :] = applied
            start = residual[at : at + 8, :]
            terms = (start * centre, centre * applied, start * start, start * applied, applied * applied)
            parts = [part + term for part, term in zip(parts, terms)]
    lane = lax.broadcasted_iota(jnp.int32, (1, LANES), 1)
    row = jnp.zeros((1, LANES), jnp.float32)
    for index, part in enumerate(parts):
        row = jnp.where(lane == index, jnp.sum(part), row)
    for copy in range(sums.shape[0]):
        sums[copy] = row


def add_kernel(received, out):
    total = received[0]
    for index in range(1, received.shape[0]):
        total = total + received[index]
    for copy in range(out.shape[0]):
        out[copy] = total


def finish_kernel(received, residual, direction, image, solution, left, norm):
    total = received[0]
    for index in range(1, received.shape[0]):
        total = total + received[index]
    lane = lax.broadcasted_iota(jnp.int32, (1, LANES), 1)
    along, curvature, old_square, cross_term, image_square = [
        jnp.full((8, LANES), jnp.sum(jnp.where(lane == index, total, 0.0)), jnp.float32) for index in range(5)
    ]
    step_size = along / curvature
    for row in range(0, 512, 8):
        solution[row : row + 8, :] = step_size * direction[row : row + 8, :]
        left[row : row + 8, :] = residual[row : row + 8, :] - step_size * image[row : row + 8, :]
    norm[...] = jnp.sqrt(old_square - 2.0 * step_size * cross_term + step_size * step_size * image_square)


def swap(block, distance, offset, keep=lambda low: True):
    count = lax.axis_size(AXES)
    route = []
    for low in range(count - distance):
        if (low - offset) % (2 * distance) < distance and keep(low):
            route += [(low, low + distance), (low + distance, low)]
    return lax.ppermute(block, AXES, route)


def exchange(rows, up, down, inner, outer, table):
    row_length = lax.axis_size("row")
    crosses = lambda low: low % row_length == row_length - 1
    message = f32(rows + rows // 2, LANES)
    near_outer = swap(outer, 1, 1, lambda low: not crosses(low))
    near_inner = swap(inner, 1, 0)
    near_across = swap(outer, 1, 1, crosses)
    (outer,) = call(functools.partial(pack_outer_kernel, rows), [message], up, down, near_inner, near_outer, table)
    far_outer = swap(outer, 2, 2)
    inner, near_outer = call(
        functools.partial(pack_inner_kernel, rows), [message, f32(rows, LANES)],
        up, down, near_inner, near_outer, near_across, table,
    )
    far_inner = swap(inner, 2, 0)
    return up, down, near_inner, near_outer, far_inner, far_outer, table


def share(block, device):
    row_length = lax.axis_size("row")
    across = swap(block, row_length, row_length)
    beside_row = swap(block, row_length, 0)
    (blocks,) = call(
        spread_kernel, [f32(row_length, 2 * BLOCK, LANES)], device, block, across, beside_row,
        in_specs=[SMEM, VMEM, VMEM, VMEM],
    )
    return lax.all_to_all(blocks, "row", 0, 0, tiled=True)


def step(right_side, counts, neighbours):
    device = lax.axis_index(AXES).astype(jnp.int32).reshape(1)
    fine = f32(512, LANES)
    faces = [f32(FINE, LANES)] * 4
    fine_ghosts = pltpu.VMEM((2 * FINE, LANES), jnp.float32)
    scratch = lambda rows: pltpu.VMEM((rows, LANES), jnp.float32)

    residual_in, *sides, table = call(
        functools.partial(start_kernel, lax.axis_size("row")), [fine, *faces, i32(TABLE_ROWS, LANES)], device, counts, right_side, neighbours,
        in_specs=[SMEM, SMEM, VMEM, VMEM],
    )
    second, *sides = call(
        smooth_kernel, [fine, *faces], residual_in, *exchange(FINE, *sides, table), scratch=[fine_ghosts]
    )
    smoothed, block, *sides = call(
        defect_kernel, [fine, f32(BLOCK, LANES), *faces],
        residual_in, second, *exchange(FINE, *sides, table), scratch=[fine_ghosts, scratch(128)],
    )
    blocks, wide_blocks, near_blocks = 2 * WIDEST + 1, 4 * REACH + 1, 2 * REACH + 1
    exchanged = exchange(FINE, *sides, table)
    direction, image, sums = call(
        image_kernel, [fine, fine, f32(lax.axis_size(AXES[1:]), 1, LANES)],
        device, residual_in, smoothed, block, share(block, device), *exchanged,
        in_specs=[SMEM] + [VMEM] * 11,
        scratch=[
            fine_ghosts, scratch(128), scratch(384), scratch(192), scratch(512),
            scratch(64 * blocks), scratch(96 * blocks), pltpu.VMEM((8 * wide_blocks, LANES), jnp.int32),
            scratch(64), scratch(96 * wide_blocks), scratch(96), *[scratch(64)] * 4,
            scratch(192 * near_blocks), scratch(192),
        ],
    )
    received = lax.all_to_all(sums, AXES[1:], 0, 0, tiled=True)
    (sums,) = call(add_kernel, [f32(lax.axis_size("outer"), 1, LANES)], received)
    received = lax.all_to_all(sums, "outer", 0, 0, tiled=True)
    solved, left, norm = call(finish_kernel, [fine, fine, f32(8, LANES)], received, residual_in, direction, image)
    return solved, left, norm[0, 0]


def solution(mesh):
    devices = mesh.devices.reshape(-1, PAIR, mesh.shape["level"])
    split = Mesh(devices, AXES)
    return jax.shard_map(
        step,
        mesh=split,
        in_specs=(P(None, AXES), P(), P(None, AXES)),
        out_specs=(P(None, AXES), P(None, AXES), P()),
        check_vma=False,
    )
```

```python
import functools

import jax
import jax.numpy as jnp
from jax import lax
from jax.experimental import pallas as pl
from jax.experimental.pallas import tpu as pltpu
from jax.sharding import Mesh
from jax.sharding import PartitionSpec as P


LANES = 128
TAIL = 64
FINE = 192
PAIR = 2
BLOCK = 72
REACH = 3
WIDEST = 8
GRANT = 8 * 1024 * 1024
AXES = ("outer", "pair", "row")
RELAX_FINE = (2.0 / 3.0) / 6.0
RELAX_COARSE = (2.0 / 3.0) / 1.5

VMEM = pl.BlockSpec(memory_space=pltpu.VMEM)
SMEM = pl.BlockSpec(memory_space=pltpu.SMEM)

LANE_ROW = 0
WINDOW_ROW = 8
FORWARD_UP = 16
FORWARD_DOWN = 24
UPPER_NEAR = 32
UPPER_FAR = 40
NEIGHBOUR_ROW = 48
CROSSES = 56
TABLE_ROWS = 64


def f32(*shape):
    return jax.ShapeDtypeStruct(shape, jnp.float32)


def i32(*shape):
    return jax.ShapeDtypeStruct(shape, jnp.int32)


def call(kernel, outs, *args, in_specs=None, out_specs=None, scratch=()):
    return pl.pallas_call(
        kernel,
        out_shape=outs,
        in_specs=in_specs or [VMEM] * len(args),
        out_specs=out_specs or [VMEM] * len(outs),
        scratch_shapes=list(scratch),
        compiler_params=pltpu.CompilerParams(vmem_limit_bytes=GRANT),
    )(*args)


def take(block, lanes):
    return jnp.take_along_axis(block, lanes, axis=1, mode="promise_in_bounds")


class Chosen:
    def __init__(self, flag, if_set, if_clear):
        self.flag, self.if_set, self.if_clear = flag, if_set, if_clear

    def __getitem__(self, at):
        return jnp.where(self.flag, self.if_set[at], self.if_clear[at])


def write_pair(table, flag_row, up, down, inner, outer, rows):
    upper = table[flag_row : flag_row + 8, :] > 0
    for row in range(0, rows, 8):
        high = up[row : row + 8, :]
        low = down[row : row + 8, :]
        inner[row : row + 8, :] = jnp.where(upper, low, high)
        outer[row : row + 8, :] = jnp.where(upper, high, low)


def write_faces(values, up, down):
    up[0:64, :] = values[448:512, :]
    down[0:64, :] = values[0:64, :]
    for x in range(8):
        up[64 + 8 * x : 72 + 8 * x, :] = values[64 * x + 56 : 64 * x + 64, :]
        down[64 + 8 * x : 72 + 8 * x, :] = values[64 * x : 64 * x + 8, :]
    up[128:192, :] = values[pl.ds(7, 64, stride=8), :]
    down[128:192, :] = values[pl.ds(0, 64, stride=8), :]


def write_coarse_faces(values, at, faces, to):
    faces[to : to + 16, :] = values[at : at + 16, :]
    faces[to + 16 : to + 32, :] = values[at + 48 : at + 64, :]
    for x in range(4):
        faces[to + 32 + 4 * x : to + 36 + 4 * x, :] = values[at + 16 * x : at + 16 * x + 4, :]
        faces[to + 48 + 4 * x : to + 52 + 4 * x, :] = values[at + 16 * x + 12 : at + 16 * x + 16, :]
    faces[to + 64 : to + 80, :] = values[pl.ds(at, 16, stride=4), :]
    faces[to + 80 : to + 96, :] = values[pl.ds(at + 3, 16, stride=4), :]


def read_planes(planes, rows, block, slots, device, out):
    blocks = planes.shape[0] // (6 * rows)
    for face in range(6):
        slot = jnp.broadcast_to(slots[face : face + 1, :], (8, LANES))
        safe = jnp.maximum(slot, 0)
        lane = safe & (LANES - 1)
        distance = jnp.where(slot >= 0, jnp.abs(lax.shift_right_logical(safe, 7) - device), -1)
        for step in range(0, rows, 8):
            picked = jnp.zeros((8, LANES), jnp.float32)
            for which in range(REACH + 1):
                source = block - which if face % 2 == 0 else block + which
                if 0 <= source < blocks:
                    row = rows * (6 * source + (face ^ 1)) + step
                    picked = jnp.where(distance == which, take(planes[row : row + 8, :], lane), picked)
            out[rows * face + step : rows * face + step + 8, :] = picked


def write_rims(faces, at, ghosts, extended, to):
    for face in range(6):
        axis, side = face // 2, 3 * (face % 2)
        row = to + 32 * face
        extended[row : row + 16, :] = faces[at + 16 * face : at + 16 * face + 16, :]
        row += 16
        for other in (other for other in range(3) if other != axis):
            along = 3 - axis - other
            for lateral in (2 * other, 2 * other + 1):
                if axis < along:
                    edge = ghosts[16 * lateral + 4 * side : 16 * lateral + 4 * side + 4, :]
                else:
                    edge = ghosts[pl.ds(16 * lateral + side, 4, stride=4), :]
                extended[row : row + 4, :] = edge
                row += 4


def windows_of(table, up, down, near_inner, near_outer, far_inner, far_outer):
    near = table[UPPER_NEAR : UPPER_NEAR + 8, :] > 0
    far = table[UPPER_FAR : UPPER_FAR + 8, :] > 0
    return (
        (up, Chosen(near, near_inner, near_outer), Chosen(far, far_inner, far_outer)),
        (down, Chosen(near, near_outer, near_inner), Chosen(far, far_outer, far_inner)),
    )


def read_ghosts(table, faces, ghosts, rows):
    windows = windows_of(table, *faces)
    per_face = rows // 3
    packed = rows // 2
    for face in range(6):
        own, near, far = windows[face % 2]
        lane = jnp.broadcast_to(table[LANE_ROW + face : LANE_ROW + face + 1, :], (8, LANES))
        window = jnp.broadcast_to(table[WINDOW_ROW + face : WINDOW_ROW + face + 1, :], (8, LANES))
        is_own, is_near, is_far, is_last = [window == which for which in range(4)]
        first_half = jnp.minimum(lane, TAIL - 1)
        second_half = first_half + TAIL
        for step in range(0, per_face, 8):
            row = (face // 2) * per_face + step
            last_row = rows + row % packed
            last_lane = first_half if row < packed else second_half
            picked = jnp.where(is_last, take(far[last_row : last_row + 8, :], last_lane), 0.0)
            picked = jnp.where(is_far, take(far[row : row + 8, :], lane), picked)
            picked = jnp.where(is_near, take(near[row : row + 8, :], lane), picked)
            picked = jnp.where(is_own, take(own[row : row + 8, :], lane), picked)
            ghosts[face * per_face + step : face * per_face + step + 8, :] = picked


def beside(values, ghosts, x, y):
    sub = lax.broadcasted_iota(jnp.int32, (8, LANES), 0)
    at = 64 * x + 8 * y
    line = 8 * x + y
    centre = values[at : at + 8, :]
    below_x = values[at - 64 : at - 56, :] if x > 0 else ghosts[8 * y : 8 * y + 8, :]
    above_x = values[at + 64 : at + 72, :] if x < 7 else ghosts[64 + 8 * y : 72 + 8 * y, :]
    below_y = values[at - 8 : at, :] if y > 0 else ghosts[128 + 8 * x : 136 + 8 * x, :]
    above_y = values[at + 8 : at + 16, :] if y < 7 else ghosts[192 + 8 * x : 200 + 8 * x, :]
    below_z = jnp.where(sub == 0, ghosts[256 + line : 257 + line, :], pltpu.roll(centre, 1, 0))
    above_z = jnp.where(sub == 7, ghosts[320 + line : 321 + line, :], pltpu.roll(centre, 7, 0))
    return centre, ((above_x + below_x) + (above_y + below_y)) + (above_z + below_z)


def start_kernel(row_length, device_ref, counts_ref, right_ref, neighbours_ref, residual, up, down, inner, outer, table):
    device = device_ref[0]
    own_count = counts_ref[device]
    lane = lax.broadcasted_iota(jnp.int32, (8, LANES), 1)
    live = lane < own_count
    for row in range(0, 512, 8):
        residual[row : row + 8, :] = jnp.where(live, right_ref[row : row + 8, :], 0.0)
    write_faces(residual, up, down)
    table[UPPER_NEAR : UPPER_NEAR + 8, :] = jnp.full((8, LANES), device & 1, jnp.int32)
    table[UPPER_FAR : UPPER_FAR + 8, :] = jnp.full((8, LANES), device & 2, jnp.int32)
    place = lax.rem(device, row_length)
    crosses = jnp.where((place == 0) | (place == row_length - 1), 1, 0)
    table[CROSSES : CROSSES + 8, :] = jnp.full((8, LANES), crosses, jnp.int32)
    write_pair(table, UPPER_NEAR, up, down, inner, outer, FINE)
    slot = neighbours_ref[...]
    present = slot >= 0
    slot = jnp.where(present, slot, 0)
    distance = jnp.abs(lax.shift_right_logical(slot, 7) - device)
    offset = slot & (LANES - 1)
    face = lax.broadcasted_iota(jnp.int32, (6, LANES), 0)
    skipped = jnp.maximum(counts_ref[jnp.maximum(device - 3, 0)] - TAIL, 0)
    shifted = jnp.where((distance == 3) & (face % 2 == 0), offset - skipped, offset)
    table[LANE_ROW : LANE_ROW + 6, :] = jnp.clip(shifted, 0, LANES - 1)
    table[WINDOW_ROW : WINDOW_ROW + 6, :] = jnp.where(present, distance, -1)
    table[NEIGHBOUR_ROW : NEIGHBOUR_ROW + 6, :] = neighbours_ref[...]
    table[NEIGHBOUR_ROW + 6 : NEIGHBOUR_ROW + 8, :] = jnp.full((2, LANES), -1, jnp.int32)
    forward = jnp.maximum(counts_ref[jnp.maximum(device - 1, 0)] - TAIL, 0)
    table[FORWARD_UP : FORWARD_UP + 8, :] = (lane & (TAIL - 1)) + forward
    table[FORWARD_DOWN : FORWARD_DOWN + 8, :] = lane & (TAIL - 1)


def pack(rows, flag_row, table, up, down, near_up, near_down, message):
    half = rows // 2
    lane = lax.broadcasted_iota(jnp.int32, (8, LANES), 1)
    upper = table[UPPER_FAR : UPPER_FAR + 8, :] > 0
    downwards = upper if flag_row else jnp.logical_not(upper)
    lanes_up = table[FORWARD_UP : FORWARD_UP + 8, :]
    lanes_down = table[FORWARD_DOWN : FORWARD_DOWN + 8, :]
    lanes = jnp.where(downwards, lanes_down, lanes_up)
    own = Chosen(downwards, down, up)
    near = Chosen(downwards, near_down, near_up)
    for row in range(0, rows, 8):
        message[row : row + 8, :] = own[row : row + 8, :]
    for row in range(0, half, 8):
        first = take(near[row : row + 8, :], lanes)
        second = take(near[half + row : half + row + 8, :], lanes)
        message[rows + row : rows + row + 8, :] = jnp.where(lane < TAIL, first, second)


def pack_outer_kernel(rows, up, down, near_inner, near_outer, table, message):
    near = table[UPPER_NEAR : UPPER_NEAR + 8, :] > 0
    near_up = Chosen(near, near_inner, near_outer)
    near_down = Chosen(near, near_outer, near_inner)
    pack(rows, False, table, up, down, near_up, near_down, message)


def pack_inner_kernel(rows, up, down, near_inner, near_outer, near_across, table, message, merged):
    near = table[UPPER_NEAR : UPPER_NEAR + 8, :] > 0
    either = Chosen(table[CROSSES : CROSSES + 8, :] > 0, near_across, near_outer)
    for row in range(0, rows, 8):
        merged[row : row + 8, :] = either[row : row + 8, :]
    near_up = Chosen(near, near_inner, merged)
    near_down = Chosen(near, merged, near_inner)
    pack(rows, True, table, up, down, near_up, near_down, message)


def smooth_kernel(residual, *refs):
    *faces, table, out, out_up, out_down, out_inner, out_outer, ghosts = refs
    read_ghosts(table, faces, ghosts, FINE)
    for x in range(8):
        for y in range(8):
            centre, around = beside(residual, ghosts, x, y)
            first = RELAX_FINE * centre
            applied = 6.0 * first - RELAX_FINE * around
            at = 64 * x + 8 * y
            out[at : at + 8, :] = first + RELAX_FINE * (centre - applied)
    write_faces(out, out_up, out_down)
    write_pair(table, UPPER_NEAR, out_up, out_down, out_inner, out_outer, FINE)


def defect_kernel(residual, second, *refs):
    *faces, table, smoothed, blocks, out_up, out_down, out_inner, out_outer, ghosts, sums = refs
    read_ghosts(table, faces, ghosts, FINE)
    for big_x in range(4):
        for big_y in range(4):
            total = None
            for x in (2 * big_x, 2 * big_x + 1):
                for y in (2 * big_y, 2 * big_y + 1):
                    centre, around = beside(second, ghosts, x, y)
                    at = 64 * x + 8 * y
                    part = residual[at : at + 8, :] - (6.0 * centre - around)
                    smoothed[at : at + 8, :] = centre + RELAX_FINE * part
                    total = part if total is None else total + part
            at = 32 * big_x + 8 * big_y
            sums[at : at + 8, :] = total
    restricted = (sums[pl.ds(0, 64, stride=2), :] + sums[pl.ds(1, 64, stride=2), :]) * 0.125
    marks = table[NEIGHBOUR_ROW : NEIGHBOUR_ROW + 8, :].astype(jnp.float32)
    for copy in range(blocks.shape[0]):
        blocks[copy, 0:64, :] = restricted
        blocks[copy, 64:72, :] = marks
    write_faces(smoothed, out_up, out_down)
    write_pair(table, UPPER_NEAR, out_up, out_down, out_inner, out_outer, FINE)


def coarse_update(first, at, ghosts, low_y, high_y, low_z, high_z):
    for x in range(4):
        low_y[16 * x : 16 * x + 4, :] = ghosts[32 + 4 * x : 36 + 4 * x, :]
        high_y[16 * x + 12 : 16 * x + 16, :] = ghosts[48 + 4 * x : 52 + 4 * x, :]
    low_z[pl.ds(0, 16, stride=4), :] = ghosts[64:80, :]
    high_z[pl.ds(3, 16, stride=4), :] = ghosts[80:96, :]
    centre = first[at : at + 64, :]
    row = lax.broadcasted_iota(jnp.int32, (64, LANES), 0)
    below_x = jnp.concatenate([ghosts[0:16, :], first[at : at + 48, :]], axis=0)
    above_x = jnp.concatenate([first[at + 16 : at + 64, :], ghosts[16:32, :]], axis=0)
    below_y = jnp.where((row & 15) < 4, low_y[...], pltpu.roll(centre, 4, 0))
    above_y = jnp.where((row & 15) >= 12, high_y[...], pltpu.roll(centre, 60, 0))
    below_z = jnp.where((row & 3) == 0, low_z[...], pltpu.roll(centre, 1, 0))
    above_z = jnp.where((row & 3) == 3, high_z[...], pltpu.roll(centre, 63, 0))
    around = ((above_x + below_x) + (above_y + below_y)) + (above_z + below_z)
    return centre + (centre - RELAX_COARSE * ((6.0 * centre - around) * 0.25))


def coarse_correction(device, in_rows, across_rows, beside_rows, scratch):
    first, first_faces, slots, coarse, coarse_faces, ghosts, low_y, high_y, low_z, high_z, extended, across = scratch
    row_length = in_rows.shape[0]
    column = lax.rem(device, row_length)
    odd_row = lax.rem(device // row_length, 2)
    for index in range(2 * WIDEST + 1):
        offset = index - WIDEST
        place = column + offset
        sender = lax.rem(place + row_length, row_length)
        inside = jnp.where((place >= 0) & (place < row_length), 1, 0)
        same = jnp.where(odd_row == jnp.where(place < 0, 1, 0), 1, 0)
        is_inside = jnp.full((8, LANES), inside, jnp.int32) > 0
        is_beside = jnp.full((8, LANES), same, jnp.int32) > 0

        def rows(row):
            outside = jnp.where(is_beside, beside_rows[sender, row : row + 8, :], across_rows[sender, row : row + 8, :])
            return jnp.where(is_inside, in_rows[sender, row : row + 8, :], outside)

        for row in range(0, 64, 8):
            first[64 * index + row : 64 * index + row + 8, :] = RELAX_COARSE * rows(row)
        write_coarse_faces(first, 64 * index, first_faces, 96 * index)
        if abs(offset) <= 2 * REACH:
            to = 8 * (offset + 2 * REACH)
            slots[to : to + 8, :] = rows(64).astype(jnp.int32)
    slots_of = lambda offset: slots.at[8 * (offset + 2 * REACH) : 8 * (offset + 2 * REACH) + 8, :]
    for offset in range(-2 * REACH, 2 * REACH + 1):
        index = offset + 2 * REACH
        read_planes(first_faces, 16, offset + WIDEST, slots_of(offset), device + offset, ghosts)
        updated = coarse_update(first, 64 * (offset + WIDEST), ghosts, low_y, high_y, low_z, high_z)
        coarse[...] = updated
        write_coarse_faces(coarse, 0, coarse_faces, 96 * index)
        if offset == 0:
            first[0:64, :] = updated
    for offset in range(-REACH, REACH + 1):
        index = offset + 2 * REACH
        read_planes(coarse_faces, 16, index, slots_of(offset), device + offset, ghosts)
        write_rims(coarse_faces, 96 * index, ghosts, extended, 192 * (offset + REACH))
    read_planes(extended, 32, REACH, slots_of(0), device, across)
    return first[0:64, :]


def image_kernel(device_ref, residual, smoothed, in_rows, across_rows, beside_rows, *refs):
    *faces, table, direction, image, sums, fine_ghosts, wide, wide_across, wide_own, spread = refs[: 7 + 3 + 5]
    scratch = refs[7 + 3 + 5 :]
    coarse_faces, across = scratch[4], scratch[-1]
    own = coarse_correction(device_ref[0], in_rows, across_rows, beside_rows, scratch)
    sub = lax.broadcasted_iota(jnp.int32, (8, LANES), 0)
    for half in (0, 1):
        wide[pl.ds(half, 64, stride=2), :] = own
        wide_across[pl.ds(half, 192, stride=2), :] = across[...]
        wide_own[pl.ds(half, 96, stride=2), :] = coarse_faces[192 * REACH : 192 * REACH + 96, :]
    for x in range(8):
        for y in range(8):
            at = 64 * x + 8 * y
            source = 32 * (x // 2) + 8 * (y // 2)
            spread[at : at + 8, :] = wide[source : source + 8, :]
    for x in range(8):
        for y in range(8):
            at = 64 * x + 8 * y
            cell = 4 * (x // 2) + y // 2
            centre = spread[at : at + 8, :]
            side_x = 8 * (y // 2)
            side_y = 8 * (x // 2)
            below_x = spread[at - 64 : at - 56, :] if x > 0 else wide_across[side_x : side_x + 8, :]
            above_x = spread[at + 64 : at + 72, :] if x < 7 else wide_across[64 + side_x : 72 + side_x, :]
            below_y = spread[at - 8 : at, :] if y > 0 else wide_across[128 + side_y : 136 + side_y, :]
            above_y = spread[at + 8 : at + 16, :] if y < 7 else wide_across[192 + side_y : 200 + side_y, :]
            below_z = jnp.where(sub == 0, across[128 + cell : 129 + cell, :], pltpu.roll(centre, 1, 0))
            above_z = jnp.where(sub == 7, across[160 + cell : 161 + cell, :], pltpu.roll(centre, 7, 0))
            around = ((above_x + below_x) + (above_y + below_y)) + (above_z + below_z)
            change = centre - RELAX_FINE * (6.0 * centre - around)
            direction[at : at + 8, :] = smoothed[at : at + 8, :] + change
    read_ghosts(table, faces, fine_ghosts, FINE)
    for face in range(6):
        for i in range(8):
            line = i // 2
            centre = wide_across[64 * face + 8 * line : 64 * face + 8 * line + 8, :]
            below = 64 * face + (8 * ((i - 1) // 2) if i > 0 else 32)
            above = 64 * face + (8 * ((i + 1) // 2) if i < 7 else 40)
            low = across[32 * face + 24 + line : 32 * face + 25 + line, :]
            high = across[32 * face + 28 + line : 32 * face + 29 + line, :]
            around = wide_across[below : below + 8, :] + wide_across[above : above + 8, :]
            around = around + jnp.where(sub == 0, low, pltpu.roll(centre, 1, 0))
            around = around + jnp.where(sub == 7, high, pltpu.roll(centre, 7, 0))
            around = around + wide_own[32 * face + 8 * line : 32 * face + 8 * line + 8, :]
            at = 64 * face + 8 * i
            change = centre - RELAX_FINE * (5.0 * centre - around)
            present = jnp.broadcast_to(table[WINDOW_ROW + face : WINDOW_ROW + face + 1, :], (8, LANES)) >= 0
            fine_ghosts[at : at + 8, :] = fine_ghosts[at : at + 8, :] + jnp.where(present, change, 0.0)
    zero = jnp.zeros((8, LANES), jnp.float32)
    parts = [zero] * 5
    for x in range(8):
        for y in range(8):
            centre, around = beside(direction, fine_ghosts, x, y)
            at = 64 * x + 8 * y
            applied = 6.0 * centre - around
            image[at : at + 8, :] = applied
            start = residual[at : at + 8, :]
            terms = (start * centre, centre * applied, start * start, start * applied, applied * applied)
            parts = [part + term for part, term in zip(parts, terms)]
    lane = lax.broadcasted_iota(jnp.int32, (1, LANES), 1)
    row = jnp.zeros((1, LANES), jnp.float32)
    for index, part in enumerate(parts):
        row = jnp.where(lane == index, jnp.sum(part), row)
    for copy in range(sums.shape[0]):
        sums[copy] = row


def add_kernel(received, out):
    total = received[0]
    for index in range(1, received.shape[0]):
        total = total + received[index]
    for copy in range(out.shape[0]):
        out[copy] = total


def finish_kernel(received, residual, direction, image, solution, left, norm):
    total = received[0]
    for index in range(1, received.shape[0]):
        total = total + received[index]
    lane = lax.broadcasted_iota(jnp.int32, (1, LANES), 1)
    along, curvature, old_square, cross_term, image_square = [
        jnp.full((8, LANES), jnp.sum(jnp.where(lane == index, total, 0.0)), jnp.float32) for index in range(5)
    ]
    step_size = along / curvature
    for row in range(0, 512, 8):
        solution[row : row + 8, :] = step_size * direction[row : row + 8, :]
        left[row : row + 8, :] = residual[row : row + 8, :] - step_size * image[row : row + 8, :]
    norm[...] = jnp.sqrt(old_square - 2.0 * step_size * cross_term + step_size * step_size * image_square)


def swap(block, distance, offset, keep=lambda low: True):
    count = lax.axis_size(AXES)
    route = []
    for low in range(count - distance):
        if (low - offset) % (2 * distance) < distance and keep(low):
            route += [(low, low + distance), (low + distance, low)]
    return lax.ppermute(block, AXES, route)


def exchange(rows, up, down, inner, outer, table):
    row_length = lax.axis_size("row")
    crosses = lambda low: low % row_length == row_length - 1
    message = f32(rows + rows // 2, LANES)
    near_outer = swap(outer, 1, 1, lambda low: not crosses(low))
    near_inner = swap(inner, 1, 0)
    near_across = swap(outer, 1, 1, crosses)
    (outer,) = call(functools.partial(pack_outer_kernel, rows), [message], up, down, near_inner, near_outer, table)
    far_outer = swap(outer, 2, 2)
    inner, near_outer = call(
        functools.partial(pack_inner_kernel, rows), [message, f32(rows, LANES)],
        up, down, near_inner, near_outer, near_across, table,
    )
    far_inner = swap(inner, 2, 0)
    return up, down, near_inner, near_outer, far_inner, far_outer, table


def share(blocks):
    row_length = lax.axis_size("row")
    in_rows = lax.all_to_all(blocks, "row", 0, 0, tiled=True)
    across_rows = swap(in_rows, row_length, row_length)
    beside_rows = swap(in_rows, row_length, 0)
    return in_rows, across_rows, beside_rows


def step(right_side, counts, neighbours):
    device = lax.axis_index(AXES).astype(jnp.int32).reshape(1)
    fine = f32(512, LANES)
    faces = [f32(FINE, LANES)] * 4
    fine_ghosts = pltpu.VMEM((2 * FINE, LANES), jnp.float32)
    scratch = lambda rows: pltpu.VMEM((rows, LANES), jnp.float32)

    residual_in, *sides, table = call(
        functools.partial(start_kernel, lax.axis_size("row")), [fine, *faces, i32(TABLE_ROWS, LANES)], device, counts, right_side, neighbours,
        in_specs=[SMEM, SMEM, VMEM, VMEM],
    )
    second, *sides = call(
        smooth_kernel, [fine, *faces], residual_in, *exchange(FINE, *sides, table), scratch=[fine_ghosts]
    )
    smoothed, blocks, *sides = call(
        defect_kernel, [fine, f32(lax.axis_size("row"), BLOCK, LANES), *faces],
        residual_in, second, *exchange(FINE, *sides, table), scratch=[fine_ghosts, scratch(128)],
    )
    all_blocks, wide_blocks, near_blocks = 2 * WIDEST + 1, 4 * REACH + 1, 2 * REACH + 1
    exchanged = exchange(FINE, *sides, table)
    direction, image, sums = call(
        image_kernel, [fine, fine, f32(lax.axis_size(AXES[1:]), 1, LANES)],
        device, residual_in, smoothed, *share(blocks), *exchanged,
        in_specs=[SMEM] + [VMEM] * 12,
        scratch=[
            fine_ghosts, scratch(128), scratch(384), scratch(192), scratch(512),
            scratch(64 * all_blocks), scratch(96 * all_blocks), pltpu.VMEM((8 * wide_blocks, LANES), jnp.int32),
            scratch(64), scratch(96 * wide_blocks), scratch(96), *[scratch(64)] * 4,
            scratch(192 * near_blocks), scratch(192),
        ],
    )
    received = lax.all_to_all(sums, AXES[1:], 0, 0, tiled=True)
    (sums,) = call(add_kernel, [f32(lax.axis_size("outer"), 1, LANES)], received)
    received = lax.all_to_all(sums, "outer", 0, 0, tiled=True)
    solved, left, norm = call(finish_kernel, [fine, fine, f32(8, LANES)], received, residual_in, direction, image)
    return solved, left, norm[0, 0]


def solution(mesh):
    devices = mesh.devices.reshape(-1, PAIR, mesh.shape["level"])
    split = Mesh(devices, AXES)
    return jax.shard_map(
        step,
        mesh=split,
        in_specs=(P(None, AXES), P(), P(None, AXES)),
        out_specs=(P(None, AXES), P(None, AXES), P()),
        check_vma=False,
    )
```

```python
import functools

import jax
import jax.numpy as jnp
from jax import lax
from jax.experimental import pallas as pl
from jax.experimental.pallas import tpu as pltpu
from jax.sharding import Mesh
from jax.sharding import PartitionSpec as P


LANES = 128
TAIL = 64
FINE = 192
PAIR = 2
BLOCK = 72
REACH = 3
WIDEST = 8
GRANT = 8 * 1024 * 1024
AXES = ("outer", "pair", "row")
RELAX_FINE = (2.0 / 3.0) / 6.0
RELAX_COARSE = (2.0 / 3.0) / 1.5

VMEM = pl.BlockSpec(memory_space=pltpu.VMEM)
SMEM = pl.BlockSpec(memory_space=pltpu.SMEM)

LANE_ROW = 0
WINDOW_ROW = 8
FORWARD_UP = 16
FORWARD_DOWN = 24
UPPER_NEAR = 32
UPPER_FAR = 40
NEIGHBOUR_ROW = 48
CROSSES = 56
TABLE_ROWS = 64


def f32(*shape):
    return jax.ShapeDtypeStruct(shape, jnp.float32)


def i32(*shape):
    return jax.ShapeDtypeStruct(shape, jnp.int32)


def call(kernel, outs, *args, in_specs=None, out_specs=None, scratch=()):
    return pl.pallas_call(
        kernel,
        out_shape=outs,
        in_specs=in_specs or [VMEM] * len(args),
        out_specs=out_specs or [VMEM] * len(outs),
        scratch_shapes=list(scratch),
        compiler_params=pltpu.CompilerParams(vmem_limit_bytes=GRANT),
    )(*args)


def take(block, lanes):
    return jnp.take_along_axis(block, lanes, axis=1, mode="promise_in_bounds")


class Chosen:
    def __init__(self, flag, if_set, if_clear):
        self.flag, self.if_set, self.if_clear = flag, if_set, if_clear

    def __getitem__(self, at):
        return jnp.where(self.flag, self.if_set[at], self.if_clear[at])


def write_pair(table, flag_row, up, down, inner, outer, rows):
    upper = table[flag_row : flag_row + 8, :] > 0
    for row in range(0, rows, 8):
        high = up[row : row + 8, :]
        low = down[row : row + 8, :]
        inner[row : row + 8, :] = jnp.where(upper, low, high)
        outer[row : row + 8, :] = jnp.where(upper, high, low)


def write_faces(values, up, down):
    up[0:64, :] = values[448:512, :]
    down[0:64, :] = values[0:64, :]
    for x in range(8):
        up[64 + 8 * x : 72 + 8 * x, :] = values[64 * x + 56 : 64 * x + 64, :]
        down[64 + 8 * x : 72 + 8 * x, :] = values[64 * x : 64 * x + 8, :]
    up[128:192, :] = values[pl.ds(7, 64, stride=8), :]
    down[128:192, :] = values[pl.ds(0, 64, stride=8), :]


def write_coarse_faces(values, at, faces, to):
    faces[to : to + 16, :] = values[at : at + 16, :]
    faces[to + 16 : to + 32, :] = values[at + 48 : at + 64, :]
    for x in range(4):
        faces[to + 32 + 4 * x : to + 36 + 4 * x, :] = values[at + 16 * x : at + 16 * x + 4, :]
        faces[to + 48 + 4 * x : to + 52 + 4 * x, :] = values[at + 16 * x + 12 : at + 16 * x + 16, :]
    faces[to + 64 : to + 80, :] = values[pl.ds(at, 16, stride=4), :]
    faces[to + 80 : to + 96, :] = values[pl.ds(at + 3, 16, stride=4), :]


def read_planes(planes, rows, block, slots, device, out):
    blocks = planes.shape[0] // (6 * rows)
    for face in range(6):
        slot = jnp.broadcast_to(slots[face : face + 1, :], (8, LANES))
        safe = jnp.maximum(slot, 0)
        lane = safe & (LANES - 1)
        distance = jnp.where(slot >= 0, jnp.abs(lax.shift_right_logical(safe, 7) - device), -1)
        for step in range(0, rows, 8):
            picked = jnp.zeros((8, LANES), jnp.float32)
            for which in range(REACH + 1):
                source = block - which if face % 2 == 0 else block + which
                if 0 <= source < blocks:
                    row = rows * (6 * source + (face ^ 1)) + step
                    picked = jnp.where(distance == which, take(planes[row : row + 8, :], lane), picked)
            out[rows * face + step : rows * face + step + 8, :] = picked


def write_rims(faces, at, ghosts, extended, to):
    for face in range(6):
        axis, side = face // 2, 3 * (face % 2)
        row = to + 32 * face
        extended[row : row + 16, :] = faces[at + 16 * face : at + 16 * face + 16, :]
        row += 16
        for other in (other for other in range(3) if other != axis):
            along = 3 - axis - other
            for lateral in (2 * other, 2 * other + 1):
                if axis < along:
                    edge = ghosts[16 * lateral + 4 * side : 16 * lateral + 4 * side + 4, :]
                else:
                    edge = ghosts[pl.ds(16 * lateral + side, 4, stride=4), :]
                extended[row : row + 4, :] = edge
                row += 4


def windows_of(table, up, down, near_inner, near_outer, far_inner, far_outer):
    near = table[UPPER_NEAR : UPPER_NEAR + 8, :] > 0
    far = table[UPPER_FAR : UPPER_FAR + 8, :] > 0
    return (
        (up, Chosen(near, near_inner, near_outer), Chosen(far, far_inner, far_outer)),
        (down, Chosen(near, near_outer, near_inner), Chosen(far, far_outer, far_inner)),
    )


def read_ghosts(table, faces, ghosts, rows):
    windows = windows_of(table, *faces)
    per_face = rows // 3
    packed = rows // 2
    for face in range(6):
        own, near, far = windows[face % 2]
        lane = jnp.broadcast_to(table[LANE_ROW + face : LANE_ROW + face + 1, :], (8, LANES))
        window = jnp.broadcast_to(table[WINDOW_ROW + face : WINDOW_ROW + face + 1, :], (8, LANES))
        is_own, is_near, is_far, is_last = [window == which for which in range(4)]
        first_half = jnp.minimum(lane, TAIL - 1)
        second_half = first_half + TAIL
        for step in range(0, per_face, 8):
            row = (face // 2) * per_face + step
            last_row = rows + row % packed
            last_lane = first_half if row < packed else second_half
            picked = jnp.where(is_last, take(far[last_row : last_row + 8, :], last_lane), 0.0)
            picked = jnp.where(is_far, take(far[row : row + 8, :], lane), picked)
            picked = jnp.where(is_near, take(near[row : row + 8, :], lane), picked)
            picked = jnp.where(is_own, take(own[row : row + 8, :], lane), picked)
            ghosts[face * per_face + step : face * per_face + step + 8, :] = picked


def beside(values, ghosts, x, y):
    sub = lax.broadcasted_iota(jnp.int32, (8, LANES), 0)
    at = 64 * x + 8 * y
    line = 8 * x + y
    centre = values[at : at + 8, :]
    below_x = values[at - 64 : at - 56, :] if x > 0 else ghosts[8 * y : 8 * y + 8, :]
    above_x = values[at + 64 : at + 72, :] if x < 7 else ghosts[64 + 8 * y : 72 + 8 * y, :]
    below_y = values[at - 8 : at, :] if y > 0 else ghosts[128 + 8 * x : 136 + 8 * x, :]
    above_y = values[at + 8 : at + 16, :] if y < 7 else ghosts[192 + 8 * x : 200 + 8 * x, :]
    below_z = jnp.where(sub == 0, ghosts[256 + line : 257 + line, :], pltpu.roll(centre, 1, 0))
    above_z = jnp.where(sub == 7, ghosts[320 + line : 321 + line, :], pltpu.roll(centre, 7, 0))
    return centre, ((above_x + below_x) + (above_y + below_y)) + (above_z + below_z)


def start_kernel(row_length, device_ref, counts_ref, right_ref, neighbours_ref, residual, up, down, inner, outer, table):
    device = device_ref[0]
    own_count = counts_ref[device]
    lane = lax.broadcasted_iota(jnp.int32, (8, LANES), 1)
    live = lane < own_count
    for row in range(0, 512, 8):
        residual[row : row + 8, :] = jnp.where(live, right_ref[row : row + 8, :], 0.0)
    write_faces(residual, up, down)
    table[UPPER_NEAR : UPPER_NEAR + 8, :] = jnp.full((8, LANES), device & 1, jnp.int32)
    table[UPPER_FAR : UPPER_FAR + 8, :] = jnp.full((8, LANES), device & 2, jnp.int32)
    place = lax.rem(device, row_length)
    crosses = jnp.where((place == 0) | (place == row_length - 1), 1, 0)
    table[CROSSES : CROSSES + 8, :] = jnp.full((8, LANES), crosses, jnp.int32)
    write_pair(table, UPPER_NEAR, up, down, inner, outer, FINE)
    slot = neighbours_ref[...]
    present = slot >= 0
    slot = jnp.where(present, slot, 0)
    distance = jnp.abs(lax.shift_right_logical(slot, 7) - device)
    offset = slot & (LANES - 1)
    face = lax.broadcasted_iota(jnp.int32, (6, LANES), 0)
    skipped = jnp.maximum(counts_ref[jnp.maximum(device - 3, 0)] - TAIL, 0)
    shifted = jnp.where((distance == 3) & (face % 2 == 0), offset - skipped, offset)
    table[LANE_ROW : LANE_ROW + 6, :] = jnp.clip(shifted, 0, LANES - 1)
    table[WINDOW_ROW : WINDOW_ROW + 6, :] = jnp.where(present, distance, -1)
    table[NEIGHBOUR_ROW : NEIGHBOUR_ROW + 6, :] = neighbours_ref[...]
    table[NEIGHBOUR_ROW + 6 : NEIGHBOUR_ROW + 8, :] = jnp.full((2, LANES), -1, jnp.int32)
    forward = jnp.maximum(counts_ref[jnp.maximum(device - 1, 0)] - TAIL, 0)
    table[FORWARD_UP : FORWARD_UP + 8, :] = (lane & (TAIL - 1)) + forward
    table[FORWARD_DOWN : FORWARD_DOWN + 8, :] = lane & (TAIL - 1)


def pack(rows, flag_row, table, up, down, near_up, near_down, message):
    half = rows // 2
    lane = lax.broadcasted_iota(jnp.int32, (8, LANES), 1)
    upper = table[UPPER_FAR : UPPER_FAR + 8, :] > 0
    downwards = upper if flag_row else jnp.logical_not(upper)
    lanes_up = table[FORWARD_UP : FORWARD_UP + 8, :]
    lanes_down = table[FORWARD_DOWN : FORWARD_DOWN + 8, :]
    lanes = jnp.where(downwards, lanes_down, lanes_up)
    own = Chosen(downwards, down, up)
    near = Chosen(downwards, near_down, near_up)
    for row in range(0, rows, 8):
        message[row : row + 8, :] = own[row : row + 8, :]
    for row in range(0, half, 8):
        first = take(near[row : row + 8, :], lanes)
        second = take(near[half + row : half + row + 8, :], lanes)
        message[rows + row : rows + row + 8, :] = jnp.where(lane < TAIL, first, second)


def pack_outer_kernel(rows, up, down, near_inner, near_outer, table, message):
    near = table[UPPER_NEAR : UPPER_NEAR + 8, :] > 0
    near_up = Chosen(near, near_inner, near_outer)
    near_down = Chosen(near, near_outer, near_inner)
    pack(rows, False, table, up, down, near_up, near_down, message)


def pack_inner_kernel(rows, up, down, near_inner, near_outer, near_across, table, message, merged):
    near = table[UPPER_NEAR : UPPER_NEAR + 8, :] > 0
    either = Chosen(table[CROSSES : CROSSES + 8, :] > 0, near_across, near_outer)
    for row in range(0, rows, 8):
        merged[row : row + 8, :] = either[row : row + 8, :]
    near_up = Chosen(near, near_inner, merged)
    near_down = Chosen(near, merged, near_inner)
    pack(rows, True, table, up, down, near_up, near_down, message)


def smooth_kernel(residual, *refs):
    *faces, table, out, out_up, out_down, out_inner, out_outer, ghosts = refs
    read_ghosts(table, faces, ghosts, FINE)
    for x in range(8):
        for y in range(8):
            centre, around = beside(residual, ghosts, x, y)
            first = RELAX_FINE * centre
            applied = 6.0 * first - RELAX_FINE * around
            at = 64 * x + 8 * y
            out[at : at + 8, :] = first + RELAX_FINE * (centre - applied)
    write_faces(out, out_up, out_down)
    write_pair(table, UPPER_NEAR, out_up, out_down, out_inner, out_outer, FINE)


def defect_kernel(residual, second, *refs):
    *faces, table, smoothed, blocks, out_up, out_down, out_inner, out_outer, ghosts, sums = refs
    read_ghosts(table, faces, ghosts, FINE)
    for big_x in range(4):
        for big_y in range(4):
            total = None
            for x in (2 * big_x, 2 * big_x + 1):
                for y in (2 * big_y, 2 * big_y + 1):
                    centre, around = beside(second, ghosts, x, y)
                    at = 64 * x + 8 * y
                    part = residual[at : at + 8, :] - (6.0 * centre - around)
                    smoothed[at : at + 8, :] = centre + RELAX_FINE * part
                    total = part if total is None else total + part
            at = 32 * big_x + 8 * big_y
            sums[at : at + 8, :] = total
    restricted = (sums[pl.ds(0, 64, stride=2), :] + sums[pl.ds(1, 64, stride=2), :]) * 0.125
    marks = table[NEIGHBOUR_ROW : NEIGHBOUR_ROW + 8, :].astype(jnp.float32)
    for copy in range(blocks.shape[0]):
        blocks[copy, 0:64, :] = restricted
        blocks[copy, 64:72, :] = marks
    write_faces(smoothed, out_up, out_down)
    write_pair(table, UPPER_NEAR, out_up, out_down, out_inner, out_outer, FINE)


def coarse_update(first, at, ghosts, low_y, high_y, low_z, high_z):
    for x in range(4):
        low_y[16 * x : 16 * x + 4, :] = ghosts[32 + 4 * x : 36 + 4 * x, :]
        high_y[16 * x + 12 : 16 * x + 16, :] = ghosts[48 + 4 * x : 52 + 4 * x, :]
    low_z[pl.ds(0, 16, stride=4), :] = ghosts[64:80, :]
    high_z[pl.ds(3, 16, stride=4), :] = ghosts[80:96, :]
    centre = first[at : at + 64, :]
    row = lax.broadcasted_iota(jnp.int32, (64, LANES), 0)
    below_x = jnp.concatenate([ghosts[0:16, :], first[at : at + 48, :]], axis=0)
    above_x = jnp.concatenate([first[at + 16 : at + 64, :], ghosts[16:32, :]], axis=0)
    below_y = jnp.where((row & 15) < 4, low_y[...], pltpu.roll(centre, 4, 0))
    above_y = jnp.where((row & 15) >= 12, high_y[...], pltpu.roll(centre, 60, 0))
    below_z = jnp.where((row & 3) == 0, low_z[...], pltpu.roll(centre, 1, 0))
    above_z = jnp.where((row & 3) == 3, high_z[...], pltpu.roll(centre, 63, 0))
    around = ((above_x + below_x) + (above_y + below_y)) + (above_z + below_z)
    return centre + (centre - RELAX_COARSE * ((6.0 * centre - around) * 0.25))


def coarse_correction(device, in_rows, across_rows, beside_rows, scratch):
    first, first_faces, slots, coarse, coarse_faces, ghosts, low_y, high_y, low_z, high_z, extended, across = scratch
    row_length = in_rows.shape[0]
    column = lax.rem(device, row_length)
    odd_row = lax.rem(device // row_length, 2)
    for index in range(2 * WIDEST + 1):
        offset = index - WIDEST
        place = column + offset
        sender = lax.rem(place + row_length, row_length)
        inside = jnp.where((place >= 0) & (place < row_length), 1, 0)
        same = jnp.where(odd_row == jnp.where(place < 0, 1, 0), 1, 0)
        is_inside = jnp.full((8, LANES), inside, jnp.int32) > 0
        is_beside = jnp.full((8, LANES), same, jnp.int32) > 0

        def rows(row):
            outside = jnp.where(is_beside, beside_rows[sender, row : row + 8, :], across_rows[sender, row : row + 8, :])
            return jnp.where(is_inside, in_rows[sender, row : row + 8, :], outside)

        for row in range(0, 64, 8):
            first[64 * index + row : 64 * index + row + 8, :] = RELAX_COARSE * rows(row)
        write_coarse_faces(first, 64 * index, first_faces, 96 * index)
        if abs(offset) <= 2 * REACH:
            to = 8 * (offset + 2 * REACH)
            slots[to : to + 8, :] = rows(64).astype(jnp.int32)
    slots_of = lambda offset: slots.at[8 * (offset + 2 * REACH) : 8 * (offset + 2 * REACH) + 8, :]
    for offset in range(-2 * REACH, 2 * REACH + 1):
        index = offset + 2 * REACH
        read_planes(first_faces, 16, offset + WIDEST, slots_of(offset), device + offset, ghosts)
        updated = coarse_update(first, 64 * (offset + WIDEST), ghosts, low_y, high_y, low_z, high_z)
        coarse[...] = updated
        write_coarse_faces(coarse, 0, coarse_faces, 96 * index)
        if offset == 0:
            first[0:64, :] = updated
    for offset in range(-REACH, REACH + 1):
        index = offset + 2 * REACH
        read_planes(coarse_faces, 16, index, slots_of(offset), device + offset, ghosts)
        write_rims(coarse_faces, 96 * index, ghosts, extended, 192 * (offset + REACH))
    read_planes(extended, 32, REACH, slots_of(0), device, across)
    return first[0:64, :]


def correct_kernel(device_ref, smoothed, in_rows, across_rows, beside_rows, direction, changes, *scratch):
    wide, wide_across, wide_own, spread, *scratch = scratch
    coarse_faces, across = scratch[4], scratch[-1]
    own = coarse_correction(device_ref[0], in_rows, across_rows, beside_rows, scratch)
    sub = lax.broadcasted_iota(jnp.int32, (8, LANES), 0)
    for half in (0, 1):
        wide[pl.ds(half, 64, stride=2), :] = own
        wide_across[pl.ds(half, 192, stride=2), :] = across[...]
        wide_own[pl.ds(half, 96, stride=2), :] = coarse_faces[192 * REACH : 192 * REACH + 96, :]
    for x in range(8):
        for y in range(8):
            at = 64 * x + 8 * y
            source = 32 * (x // 2) + 8 * (y // 2)
            spread[at : at + 8, :] = wide[source : source + 8, :]
    for x in range(8):
        for y in range(8):
            at = 64 * x + 8 * y
            cell = 4 * (x // 2) + y // 2
            centre = spread[at : at + 8, :]
            side_x = 8 * (y // 2)
            side_y = 8 * (x // 2)
            below_x = spread[at - 64 : at - 56, :] if x > 0 else wide_across[side_x : side_x + 8, :]
            above_x = spread[at + 64 : at + 72, :] if x < 7 else wide_across[64 + side_x : 72 + side_x, :]
            below_y = spread[at - 8 : at, :] if y > 0 else wide_across[128 + side_y : 136 + side_y, :]
            above_y = spread[at + 8 : at + 16, :] if y < 7 else wide_across[192 + side_y : 200 + side_y, :]
            below_z = jnp.where(sub == 0, across[128 + cell : 129 + cell, :], pltpu.roll(centre, 1, 0))
            above_z = jnp.where(sub == 7, across[160 + cell : 161 + cell, :], pltpu.roll(centre, 7, 0))
            around = ((above_x + below_x) + (above_y + below_y)) + (above_z + below_z)
            change = centre - RELAX_FINE * (6.0 * centre - around)
            direction[at : at + 8, :] = smoothed[at : at + 8, :] + change
    for face in range(6):
        for i in range(8):
            line = i // 2
            centre = wide_across[64 * face + 8 * line : 64 * face + 8 * line + 8, :]
            below = 64 * face + (8 * ((i - 1) // 2) if i > 0 else 32)
            above = 64 * face + (8 * ((i + 1) // 2) if i < 7 else 40)
            low = across[32 * face + 24 + line : 32 * face + 25 + line, :]
            high = across[32 * face + 28 + line : 32 * face + 29 + line, :]
            around = wide_across[below : below + 8, :] + wide_across[above : above + 8, :]
            around = around + jnp.where(sub == 0, low, pltpu.roll(centre, 1, 0))
            around = around + jnp.where(sub == 7, high, pltpu.roll(centre, 7, 0))
            around = around + wide_own[32 * face + 8 * line : 32 * face + 8 * line + 8, :]
            at = 64 * face + 8 * i
            changes[at : at + 8, :] = centre - RELAX_FINE * (5.0 * centre - around)


def image_kernel(residual, direction, changes, *refs):
    *faces, table, image, sums, fine_ghosts = refs
    read_ghosts(table, faces, fine_ghosts, FINE)
    for face in range(6):
        present = jnp.broadcast_to(table[WINDOW_ROW + face : WINDOW_ROW + face + 1, :], (8, LANES)) >= 0
        for at in range(64 * face, 64 * face + 64, 8):
            change = jnp.where(present, changes[at : at + 8, :], 0.0)
            fine_ghosts[at : at + 8, :] = fine_ghosts[at : at + 8, :] + change
    zero = jnp.zeros((8, LANES), jnp.float32)
    parts = [zero] * 5
    for x in range(8):
        for y in range(8):
            centre, around = beside(direction, fine_ghosts, x, y)
            at = 64 * x + 8 * y
            applied = 6.0 * centre - around
            image[at : at + 8, :] = applied
            start = residual[at : at + 8, :]
            terms = (start * centre, centre * applied, start * start, start * applied, applied * applied)
            parts = [part + term for part, term in zip(parts, terms)]
    lane = lax.broadcasted_iota(jnp.int32, (1, LANES), 1)
    row = jnp.zeros((1, LANES), jnp.float32)
    for index, part in enumerate(parts):
        row = jnp.where(lane == index, jnp.sum(part), row)
    for copy in range(sums.shape[0]):
        sums[copy] = row


def add_kernel(received, out):
    total = received[0]
    for index in range(1, received.shape[0]):
        total = total + received[index]
    for copy in range(out.shape[0]):
        out[copy] = total


def finish_kernel(received, residual, direction, image, solution, left, norm):
    total = received[0]
    for index in range(1, received.shape[0]):
        total = total + received[index]
    lane = lax.broadcasted_iota(jnp.int32, (1, LANES), 1)
    along, curvature, old_square, cross_term, image_square = [
        jnp.full((8, LANES), jnp.sum(jnp.where(lane == index, total, 0.0)), jnp.float32) for index in range(5)
    ]
    step_size = along / curvature
    for row in range(0, 512, 8):
        solution[row : row + 8, :] = step_size * direction[row : row + 8, :]
        left[row : row + 8, :] = residual[row : row + 8, :] - step_size * image[row : row + 8, :]
    root = jnp.sqrt(old_square - 2.0 * step_size * cross_term + step_size * step_size * image_square)
    norm[0] = jnp.max(root)


def swap(block, distance, offset, keep=lambda low: True):
    count = lax.axis_size(AXES)
    route = []
    for low in range(count - distance):
        if (low - offset) % (2 * distance) < distance and keep(low):
            route += [(low, low + distance), (low + distance, low)]
    return lax.ppermute(block, AXES, route)


def exchange(rows, up, down, inner, outer, table):
    row_length = lax.axis_size("row")
    crosses = lambda low: low % row_length == row_length - 1
    message = f32(rows + rows // 2, LANES)
    near_outer = swap(outer, 1, 1, lambda low: not crosses(low))
    near_inner = swap(inner, 1, 0)
    near_across = swap(outer, 1, 1, crosses)
    (outer,) = call(functools.partial(pack_outer_kernel, rows), [message], up, down, near_inner, near_outer, table)
    far_outer = swap(outer, 2, 2)
    inner, near_outer = call(
        functools.partial(pack_inner_kernel, rows), [message, f32(rows, LANES)],
        up, down, near_inner, near_outer, near_across, table,
    )
    far_inner = swap(inner, 2, 0)
    return up, down, near_inner, near_outer, far_inner, far_outer, table


def share(blocks):
    row_length = lax.axis_size("row")
    in_rows = lax.all_to_all(blocks, "row", 0, 0, tiled=True)
    across_rows = swap(in_rows, row_length, row_length)
    beside_rows = swap(in_rows, row_length, 0)
    return in_rows, across_rows, beside_rows


def step(right_side, counts, neighbours):
    device = lax.axis_index(AXES).astype(jnp.int32).reshape(1)
    fine = f32(512, LANES)
    faces = [f32(FINE, LANES)] * 4
    fine_ghosts = pltpu.VMEM((2 * FINE, LANES), jnp.float32)
    scratch = lambda rows: pltpu.VMEM((rows, LANES), jnp.float32)

    residual_in, *sides, table = call(
        functools.partial(start_kernel, lax.axis_size("row")), [fine, *faces, i32(TABLE_ROWS, LANES)], device, counts, right_side, neighbours,
        in_specs=[SMEM, SMEM, VMEM, VMEM],
    )
    second, *sides = call(
        smooth_kernel, [fine, *faces], residual_in, *exchange(FINE, *sides, table), scratch=[fine_ghosts]
    )
    smoothed, blocks, *sides = call(
        defect_kernel, [fine, f32(lax.axis_size("row"), BLOCK, LANES), *faces],
        residual_in, second, *exchange(FINE, *sides, table), scratch=[fine_ghosts, scratch(128)],
    )
    all_blocks, wide_blocks, near_blocks = 2 * WIDEST + 1, 4 * REACH + 1, 2 * REACH + 1
    exchanged = exchange(FINE, *sides, table)
    direction, changes = call(
        correct_kernel, [fine, f32(2 * FINE, LANES)], device, smoothed, *share(blocks),
        in_specs=[SMEM] + [VMEM] * 4,
        scratch=[
            scratch(128), scratch(384), scratch(192), scratch(512),
            scratch(64 * all_blocks), scratch(96 * all_blocks), pltpu.VMEM((8 * wide_blocks, LANES), jnp.int32),
            scratch(64), scratch(96 * wide_blocks), scratch(96), *[scratch(64)] * 4,
            scratch(192 * near_blocks), scratch(192),
        ],
    )
    image, sums = call(
        image_kernel, [fine, f32(lax.axis_size(AXES[1:]), 1, LANES)],
        residual_in, direction, changes, *exchanged, scratch=[fine_ghosts],
    )
    received = lax.all_to_all(sums, AXES[1:], 0, 0, tiled=True)
    (sums,) = call(add_kernel, [f32(lax.axis_size("outer"), 1, LANES)], received)
    received = lax.all_to_all(sums, "outer", 0, 0, tiled=True)
    solved, left, norm = call(
        finish_kernel, [fine, fine, f32(1)], received, residual_in, direction, image,
        out_specs=[VMEM, VMEM, SMEM],
    )
    return solved, left, norm.reshape(())


def solution(mesh):
    devices = mesh.devices.reshape(-1, PAIR, mesh.shape["level"])
    split = Mesh(devices, AXES)
    return jax.shard_map(
        step,
        mesh=split,
        in_specs=(P(None, AXES), P(), P(None, AXES)),
        out_specs=(P(None, AXES), P(None, AXES), P()),
        check_vma=False,
    )
```
